32 devices in a mesh: task: 1 (over z), row: 32 (over y, x, core).
Axes of the slice: x: 4, y: 4, z: 1, core: 2. Of those that a mesh axis runs over, the one named last changes fastest.
The devices are a block of a 4x4x8 slice.
Arguments:
- points: bfloat16 [49152, 128], P(('task', 'row'))
- vectors: bfloat16 [49152, 16], P(('task', 'row'))
- length_scale: float32 [1], P('task')
- out_scale: float32 [1], P('task')
Outputs:
- output: float32 [49152, 16], P(('task', 'row'))
All inputs are finite; a program needn't handle non-finite values.
Results may differ from the reference program's by a relative error of at most 0.001.
Values are sent between devices in bfloat16 or wider.
A program may use at most 768 MiB of HBM per device.

```python
import jax
import jax.numpy as jnp
from jax import lax

ROWS_DEV = 1536
GROUP = 32
FEAT = 128
COLS = 16
N_POINTS = GROUP * ROWS_DEV


def setup_inputs(seed: int = 0, part: int = 0) -> dict:
    base_key = jax.random.fold_in(jax.random.key(seed), part)
    key_x, key_o, key_m, key_v, key_l, key_s = jax.random.split(base_key, 6)
    base_pts = jax.random.normal(key_x, (GROUP, ROWS_DEV, FEAT), jnp.float32)
    offset = 1.6 * jax.random.normal(key_o, (GROUP, 1, FEAT), jnp.float32)
    points = (base_pts + offset).reshape(N_POINTS, FEAT).astype(jnp.bfloat16)
    block_mean = jax.random.normal(key_m, (GROUP, 1, COLS), jnp.float32)
    block_mean = block_mean - jnp.mean(block_mean, axis=0, keepdims=True)
    noise_val = 0.5 * jax.random.normal(key_v, (GROUP, ROWS_DEV, COLS), jnp.float32)
    vectors = (block_mean + noise_val).reshape(N_POINTS, COLS).astype(jnp.bfloat16)
    ell_ratio = jax.random.uniform(key_l, (1,), jnp.float32, 0.8, 1.25)
    length_scale = jnp.sqrt(2.0 * FEAT * ell_ratio)
    out_scale = jax.random.uniform(key_s, (1,), jnp.float32, 1.0, 2.0) / ROWS_DEV
    return {"points": points, "vectors": vectors, "length_scale": length_scale, "out_scale": out_scale}


def kernel_tile(x_rows, x_cols, length_scale, out_scale):
    norm_rows = jnp.sum(jnp.square(x_rows.astype(jnp.float32)), axis=1)
    norm_cols = jnp.sum(jnp.square(x_cols.astype(jnp.float32)), axis=1)
    gram_mat = jnp.dot(x_rows, x_cols.T, preferred_element_type=jnp.float32)
    sq_dist = jnp.maximum(norm_rows[:, None] + norm_cols[None, :] - 2.0 * gram_mat, 0.0)
    return (out_scale * jnp.exp(-sq_dist / (2.0 * length_scale * length_scale))).astype(jnp.bfloat16)


def kernel_apply(points, vectors, length_scale, out_scale):
    x_blocks = points.reshape(GROUP, ROWS_DEV, FEAT)
    v_blocks = vectors.reshape(GROUP, ROWS_DEV, COLS)

    def row_block(x_rows):
        def col_step(running, col_pair):
            x_cols, v_cols = col_pair
            kern_tile = kernel_tile(x_rows, x_cols, length_scale, out_scale)
            return running + jnp.dot(kern_tile, v_cols, preferred_element_type=jnp.float32), None

        running, _ = lax.scan(col_step, jnp.zeros((ROWS_DEV, COLS), jnp.float32), (x_blocks, v_blocks))
        return running

    return lax.map(row_block, x_blocks).reshape(N_POINTS, COLS)


def reference(points, vectors, length_scale, out_scale):
    first_pass = kernel_apply(points, vectors, length_scale, out_scale).astype(jnp.bfloat16)
    return kernel_apply(points, first_pass, length_scale, out_scale)
```

```python
import functools

import jax
import jax.numpy as jnp
from jax import lax
from jax.experimental import pallas as pl
from jax.experimental.pallas import tpu as pltpu
from jax.sharding import PartitionSpec as P

BF16 = jnp.bfloat16
F32 = jnp.float32
LOG2E = 1.4426950408889634
COL_TILE = 512
ROW_TILE = 768


def split3(val):
    high = val.astype(BF16).astype(F32)
    mid = (val - high).astype(BF16).astype(F32)
    low = (val - high) - mid
    return high, mid, low


def pass_kernel(scal_ref, own_ref, vis_ref, vt_ref, out_ref):
    rows, feat2 = vis_ref.shape
    own = own_ref.shape[1]
    coef = scal_ref[0]
    scale = scal_ref[1]
    cap = jnp.full((ROW_TILE, COL_TILE), scale, F32).astype(BF16)

    @pl.when(pl.program_id(0) == 0)
    def _():
        out_ref[...] = jnp.zeros_like(out_ref)

    for col in range(0, own, COL_TILE):
        total = out_ref[:, pl.ds(col, COL_TILE)]
        for row in range(0, rows, ROW_TILE):
            neg_dist = jnp.dot(vis_ref[pl.ds(row, ROW_TILE), :], own_ref[:, pl.ds(col, COL_TILE)], preferred_element_type=F32)
            tile = jnp.minimum((jnp.exp2(neg_dist * coef) * scale).astype(BF16), cap)
            total = total + jnp.dot(vt_ref[:, pl.ds(row, ROW_TILE)], tile, preferred_element_type=F32)
        out_ref[:, pl.ds(col, COL_TILE)] = total


def kernel_pass(scal, own_side, vis_side, vt_all):
    n_all, feat2 = vis_side.shape
    own = own_side.shape[1]
    n_col = vt_all.shape[0]
    return pl.pallas_call(
        pass_kernel,
        grid=(n_all // own,),
        in_specs=[
            pl.BlockSpec(memory_space=pltpu.SMEM),
            pl.BlockSpec((feat2, own), lambda i: (0, 0)),
            pl.BlockSpec((own, feat2), lambda i: (i, 0)),
            pl.BlockSpec((n_col, own), lambda i: (0, i)),
        ],
        out_specs=pl.BlockSpec((n_col, own), lambda i: (0, 0)),
        out_shape=jax.ShapeDtypeStruct((n_col, own), F32),
        cost_estimate=pl.CostEstimate(flops=2 * n_all * own * feat2, bytes_accessed=2 * n_all * feat2, transcendentals=n_all * own),
        name="kernel_pass",
    )(scal, own_side, vis_side, vt_all)


def solution(mesh):
    def local_program(x_loc, v_loc, length_scale, out_scale):
        ell, scale = length_scale[0], out_scale[0]
        shrink = jnp.where(ell > 2.0**64, 2.0**-70, jnp.where(ell > 2.0**32, 2.0**-32, 1.0)).astype(F32)
        ell = ell * shrink
        coef = LOG2E / (2.0 * ell * ell)
        scal = jnp.stack([coef, scale])
        x_f = x_loc.astype(F32) * shrink
        parts = split3(jnp.sum(jnp.square(x_f), axis=1))
        rows = x_loc.shape[0]
        one = jnp.ones((rows,), F32)
        pad = jnp.zeros((rows, x_loc.shape[1] - 6), F32)
        vis = jnp.concatenate([x_f, jnp.stack([*parts, one, one, one], axis=1), pad], axis=1).astype(BF16)
        own = jnp.concatenate([2.0 * x_f, jnp.stack([-one, -one, -one, *(-p for p in parts)], axis=1), pad], axis=1).astype(BF16).T
        vis_all = lax.all_gather(vis, "row", axis=0, tiled=True)
        vt_all = lax.all_gather(v_loc, "row", axis=0, tiled=True).T
        first = kernel_pass(scal, own, vis_all, vt_all).astype(BF16)
        yt_all = lax.all_gather(first, "row", axis=1, tiled=True)
        return kernel_pass(scal, own, vis_all, yt_all).T

    row_spec = P(("task", "row"), None)
    return jax.shard_map(local_program, mesh=mesh, in_specs=(row_spec, row_spec, P("task"), P("task")), out_specs=row_spec, check_vma=False)
```

```python
import math

import jax
import jax.numpy as jnp
from jax import lax
from jax.experimental import pallas as pl
from jax.experimental.pallas import tpu as pltpu
from jax.sharding import PartitionSpec as P

BF16 = jnp.bfloat16
F32 = jnp.float32
LOG2E = 1.4426950408889634
TILE = 512
LANES = 128
LAG = 1
STEP = ((1, 0), (0, 1), (-1, 0), (0, -1))
WAVES = (
    (0, 0, 1, 0),
    (2, 0, -1, 0),
    (3, 0, 0, 1),
    (1, 0, 0, -1),
    (0, 1, 2, 0),
    (3, 1, 1, 1),
    (1, 1, 1, -1),
    (3, 2, -1, 1),
    (1, 2, -1, -1),
    (3, 3, 0, 2),
    (3, 5, 2, 1),
    (1, 5, 2, -1),
    (3, 6, 1, 2),
    (3, 8, -1, 2),
    (3, 11, 2, 2),
)
AHEAD = 4


def split3(val):
    high = val.astype(BF16).astype(F32)
    mid = (val - high).astype(BF16).astype(F32)
    low = (val - high) - mid
    return high, mid, low


def make_kernel(n_row, own):
    side = math.isqrt(n_row // 2)
    n_slot = side * side
    quarter = own // 4
    n_c, n_r = own // TILE, own // TILE
    units = [(c, r) for c in range(n_c) for r in range(n_r)]
    n_u = len(units)

    def kernel(
        scal_ref, x_ref, vt_ref, out_ref, xbuf, abuf, vbuf, ybuf, wbuf, total,
        load_sem, send_sem, recv_sem, sib_send, sib_recv, ysend_sem, yrecv_sem, ysib_send, ysib_recv,
    ):
        me = lax.axis_index("row")
        core, chip = me % 2, me // 2
        cx, cy = chip % side, chip // side

        def chip_id(dx, dy):
            return {"row": (((cy + dy + side) % side) * side + (cx + dx + side) % side) * 2 + core}

        sibling = {"row": chip * 2 + 1 - core}

        load_x = pltpu.make_async_copy(x_ref, xbuf.at[0, 0], load_sem.at[0])
        load_v = pltpu.make_async_copy(vt_ref, vbuf.at[0, 1, pl.ds(0, 16)], load_sem.at[1])
        load_x.start()
        load_v.start()

        barrier = pltpu.get_barrier_semaphore()
        for k in range(1, n_slot):
            pl.semaphore_signal(barrier, inc=1, device_id=chip_id(k % side, k // side))
        pl.semaphore_signal(barrier, inc=1, device_id=sibling)

        coef, scale, shrink2 = scal_ref[0], scal_ref[1], scal_ref[2]
        cap = jnp.full((TILE, TILE), scale, F32).astype(BF16)
        wbuf[pl.ds(LANES + 16, LANES - 16), :] = jnp.zeros((LANES - 16, own), BF16)

        load_x.wait()
        load_v.wait()
        row_idx = lax.broadcasted_iota(jnp.int32, (16, LANES), 0)
        for r in range(own // LANES):
            x_t = xbuf[0, 0, pl.ds(r * LANES, LANES), :].astype(F32).T
            norm = jnp.sum(x_t * x_t, axis=0, keepdims=True) * shrink2
            parts = [jnp.broadcast_to(p, (16, LANES)) for p in split3(norm)]
            vis = jnp.where(row_idx < 6, 1.0, 0.0)
            mine = jnp.where(row_idx < 3, -1.0, 0.0)
            for i, part in enumerate(parts):
                vis = jnp.where(row_idx == i, part, vis)
                mine = jnp.where(row_idx == i + 3, -part, mine)
            vbuf[0, 1, pl.ds(16, 16), pl.ds(r * LANES, LANES)] = vis.astype(BF16)
            wbuf[pl.ds(0, LANES), pl.ds(r * LANES, LANES)] = (x_t * (2.0 * shrink2)).astype(BF16)
            wbuf[pl.ds(LANES, 16), pl.ds(r * LANES, LANES)] = mine.astype(BF16)

        def wave_copies(wave):
            rel, src, _, _ = WAVES[wave]
            copies = []
            for d in range(4):
                q = (d + rel) % 4
                target = chip_id(*STEP[d])
                rows = pl.ds(q * quarter, quarter)
                copies.append(pltpu.make_async_remote_copy(
                    xbuf.at[0, src, rows], xbuf.at[0, wave + 1, rows], send_sem.at[wave % AHEAD, q, 0], recv_sem.at[wave, q, 0], device_id=target))
                copies.append(pltpu.make_async_remote_copy(
                    vbuf.at[0, src + 1, :, rows], vbuf.at[0, wave + 2, :, rows], send_sem.at[wave % AHEAD, q, 1], recv_sem.at[wave, q, 1], device_id=target))
            return copies

        def piece_copies(slot):
            copies = []
            for q in range(4):
                rows = pl.ds(q * quarter, quarter)
                sem = (slot - 1) % AHEAD
                copies.append(pltpu.make_async_remote_copy(
                    xbuf.at[0, slot, rows], xbuf.at[0, slot, rows], send_sem.at[sem, q, 0], recv_sem.at[slot - 1, q, 0], device_id=sibling))
                copies.append(pltpu.make_async_remote_copy(
                    vbuf.at[0, slot + 1, :, rows], vbuf.at[0, slot + 1, :, rows], send_sem.at[sem, q, 1], recv_sem.at[slot - 1, q, 1], device_id=sibling))
            return copies

        def sibling_copies(slot):
            return (
                pltpu.make_async_remote_copy(xbuf.at[0, slot], xbuf.at[1, slot], sib_send.at[0], sib_recv.at[slot, 0], device_id=sibling),
                pltpu.make_async_remote_copy(vbuf.at[0, slot + 1], vbuf.at[1, slot + 1], sib_send.at[1], sib_recv.at[slot, 1], device_id=sibling),
            )

        def y_piece_copy(slot, q, target):
            rows = pl.ds(q * quarter, quarter)
            return pltpu.make_async_remote_copy(
                ybuf.at[0, 1, :, rows], ybuf.at[0, slot + 1, :, rows], ysend_sem.at[slot - 1, q], yrecv_sem.at[slot - 1, q], device_id=target)

        def y_sibling_copy(slot):
            return pltpu.make_async_remote_copy(ybuf.at[0, slot + 1], ybuf.at[1, slot + 1], ysib_send.at[0], ysib_recv.at[slot], device_id=sibling)

        def widen(which, slot, r):
            for lane in range(r * TILE, (r + 1) * TILE, LANES):
                rows = vbuf[which, slot + 1, pl.ds(16, 16), pl.ds(lane, LANES)].astype(F32)
                full = jnp.concatenate([rows, jnp.zeros((LANES - 16, LANES), F32)], axis=0)
                abuf[which, slot, pl.ds(lane, LANES), :] = full.T.astype(BF16)

        def block(buf, which, slot, first):
            gram = {}
            if first:
                widen(which, slot, 0)
            for u in range(n_u + LAG):
                if first and u + 1 < n_r:
                    widen(which, slot, u + 1)
                if u < n_u:
                    c, r = units[u]
                    rows = pl.ds(r * TILE, TILE)
                    lhs = jnp.concatenate([xbuf[which, slot, rows, :], abuf[which, slot, rows, :]], axis=1)
                    gram[u] = jnp.dot(lhs, wbuf[:, pl.ds(c * TILE, TILE)], preferred_element_type=F32)
                if u >= LAG:
                    c, r = units[u - LAG]
                    tile = jnp.minimum((jnp.exp2(gram.pop(u - LAG) * coef) * scale).astype(BF16), cap)
                    lhs = buf[which, slot + 1, pl.ds(0, 16), pl.ds(r * TILE, TILE)]
                    total[:, pl.ds(c * TILE, TILE)] += jnp.dot(lhs, tile, preferred_element_type=F32)

        total[...] = jnp.zeros_like(total)
        pl.semaphore_wait(barrier, n_slot)
        for copy in sibling_copies(0):
            copy.start()
        for wave in range(AHEAD):
            for copy in wave_copies(wave):
                copy.start()

        def first_step(slot, carry):
            @pl.when(slot > 0)
            def _():
                for copy in piece_copies(slot):
                    copy.wait()
                for copy in sibling_copies(slot):
                    copy.wait_send()
                    copy.start()

            for wave in range(AHEAD, n_slot - 1):
                @pl.when(slot == wave - AHEAD + 1)
                def _():
                    for copy in wave_copies(wave):
                        copy.start()

            block(vbuf, 0, slot, True)
            for copy in sibling_copies(slot):
                copy.wait_recv()
            block(vbuf, 1, slot, True)
            return carry

        lax.fori_loop(0, n_slot, first_step, 0)
        ybuf[0, 1] = total[...].astype(BF16)
        total[...] = jnp.zeros_like(total)
        for copy in sibling_copies(n_slot - 1):
            copy.wait_send()

        y_sibling_copy(0).start()
        for wave, (_, _, prim, sec) in enumerate(WAVES):
            for q in range(4):
                (px, py), (sx, sy) = STEP[q], STEP[(q + 1) % 4]
                y_piece_copy(wave + 1, q, chip_id((prim * px + sec * sx) % side, (prim * py + sec * sy) % side)).start()

        def second_step(slot, carry):
            @pl.when(slot > 0)
            def _():
                for q in range(4):
                    y_piece_copy(slot, q, sibling).wait()
                y_sibling_copy(slot).wait_send()
                y_sibling_copy(slot).start()

            block(ybuf, 0, slot, False)
            y_sibling_copy(slot).wait_recv()
            block(ybuf, 1, slot, False)
            return carry

        lax.fori_loop(0, n_slot, second_step, 0)
        out_ref[...] = total[...]
        y_sibling_copy(n_slot - 1).wait_send()

    return kernel, n_slot


def both_passes(n_row, scal, x_loc, vt_loc):
    own, feat = x_loc.shape
    n_col = vt_loc.shape[0]
    kernel, n_slot = make_kernel(n_row, own)
    dma = pltpu.SemaphoreType.DMA
    return pl.pallas_call(
        kernel,
        in_specs=[pl.BlockSpec(memory_space=pltpu.SMEM), pl.BlockSpec(memory_space=pl.ANY), pl.BlockSpec(memory_space=pl.ANY)],
        out_specs=pl.BlockSpec(memory_space=pltpu.VMEM),
        out_shape=jax.ShapeDtypeStruct((n_col, own), F32),
        scratch_shapes=[
            pltpu.VMEM((2, n_slot, own, feat), BF16),
            pltpu.VMEM((2, n_slot, own, feat), BF16),
            pltpu.VMEM((2, n_slot + 1, 32, own), BF16),
            pltpu.VMEM((2, n_slot + 1, n_col, own), BF16),
            pltpu.VMEM((2 * feat, own), BF16),
            pltpu.VMEM((n_col, own), F32),
            dma((2,)),
            dma((AHEAD, 4, 2)),
            dma((n_slot - 1, 4, 2)),
            dma((2,)),
            dma((n_slot, 2)),
            dma((n_slot - 1, 4)),
            dma((n_slot - 1, 4)),
            dma((1,)),
            dma((n_slot,)),
        ],
        compiler_params=pltpu.CompilerParams(collective_id=0, has_side_effects=True, vmem_limit_bytes=64000000),
        name="both_passes",
    )(scal, x_loc, vt_loc)


def solution(mesh):
    def local_program(x_loc, v_loc, length_scale, out_scale):
        ell, scale = length_scale[0], out_scale[0]
        shrink = jnp.where(ell > 2.0**64, 2.0**-70, jnp.where(ell > 2.0**32, 2.0**-32, 1.0)).astype(F32)
        ell = ell * shrink
        scal = jnp.stack([LOG2E / (2.0 * ell * ell), scale, shrink * shrink])
        return both_passes(mesh.shape["row"], scal, x_loc, v_loc.T).T

    row_spec = P(("task", "row"), None)
    return jax.shard_map(local_program, mesh=mesh, in_specs=(row_spec, row_spec, P("task"), P("task")), out_specs=row_spec, check_vma=False)
```

```python
import math

import jax
import jax.numpy as jnp
from jax import lax
from jax.experimental import pallas as pl
from jax.experimental.pallas import tpu as pltpu
from jax.sharding import PartitionSpec as P

BF16 = jnp.bfloat16
F32 = jnp.float32
LOG2E = 1.4426950408889634
TILE = 512
LANES = 128
LAG = 1
PAD = 128
STEP = ((1, 0), (0, 1), (-1, 0), (0, -1))
WAVES = (
    (0, 0, 1, 0),
    (2, 0, -1, 0),
    (3, 0, 0, 1),
    (1, 0, 0, -1),
    (0, 1, 2, 0),
    (3, 1, 1, 1),
    (1, 1, 1, -1),
    (3, 2, -1, 1),
    (1, 2, -1, -1),
    (3, 3, 0, 2),
    (3, 5, 2, 1),
    (1, 5, 2, -1),
    (3, 6, 1, 2),
    (3, 8, -1, 2),
    (3, 11, 2, 2),
)
AHEAD = 4


def split3(val):
    high = val.astype(BF16).astype(F32)
    mid = (val - high).astype(BF16).astype(F32)
    low = (val - high) - mid
    return high, mid, low


def make_kernel(n_row, own):
    side = math.isqrt(n_row // 2)
    n_slot = side * side
    quarter = own // 4
    n_c, n_r = own // TILE, own // TILE
    units = [(c, r) for c in range(n_c) for r in range(n_r)]
    n_u = len(units)

    def kernel(
        scal_ref, x_ref, vt_ref, out_ref, xbuf, abuf, vbuf, ybuf, wbuf, total,
        load_sem, send_sem, recv_sem, sib_send, sib_recv, ysend_sem, yrecv_sem, ysib_send, ysib_recv,
    ):
        me = lax.axis_index("row")
        core, chip = me % 2, me // 2
        cx, cy = chip % side, chip // side

        def chip_id(dx, dy):
            return {"row": (((cy + dy + side) % side) * side + (cx + dx + side) % side) * 2 + core}

        sibling = {"row": chip * 2 + 1 - core}

        load_x = pltpu.make_async_copy(x_ref, xbuf.at[0, 0], load_sem.at[0])
        load_v = pltpu.make_async_copy(vt_ref, vbuf.at[0, 1, pl.ds(0, 16)], load_sem.at[1])
        load_x.start()
        load_v.start()

        barrier = pltpu.get_barrier_semaphore()
        for k in range(1, n_slot):
            pl.semaphore_signal(barrier, inc=1, device_id=chip_id(k % side, k // side))
        pl.semaphore_signal(barrier, inc=1, device_id=sibling)

        coef, scale, shrink2 = scal_ref[0], scal_ref[1], scal_ref[2]
        cap = jnp.full((TILE, TILE), scale, F32).astype(BF16)
        wbuf[pl.ds(LANES + 16, LANES - 16), :] = jnp.zeros((LANES - 16, own), BF16)

        load_x.wait()
        load_v.wait()
        row_idx = lax.broadcasted_iota(jnp.int32, (16, LANES), 0)
        for r in range(own // LANES):
            x_t = xbuf[0, 0, pl.ds(r * LANES, LANES), :].astype(F32).T
            norm = jnp.sum(x_t * x_t, axis=0, keepdims=True) * shrink2
            parts = [jnp.broadcast_to(p, (16, LANES)) for p in split3(norm)]
            vis = jnp.where(row_idx < 6, 1.0, 0.0)
            mine = jnp.where(row_idx < 3, -1.0, 0.0)
            for i, part in enumerate(parts):
                vis = jnp.where(row_idx == i, part, vis)
                mine = jnp.where(row_idx == i + 3, -part, mine)
            vbuf[0, 1, pl.ds(16, 16), pl.ds(r * LANES, LANES)] = vis.astype(BF16)
            wbuf[pl.ds(0, LANES), pl.ds(r * LANES, LANES)] = (x_t * (2.0 * shrink2)).astype(BF16)
            wbuf[pl.ds(LANES, 16), pl.ds(r * LANES, LANES)] = mine.astype(BF16)

        def wave_copies(wave):
            rel, src, _, _ = WAVES[wave]
            copies = []
            for d in range(4):
                q = (d + rel) % 4
                target = chip_id(*STEP[d])
                rows = pl.ds(q * quarter, quarter)
                copies.append(pltpu.make_async_remote_copy(
                    xbuf.at[0, src, rows], xbuf.at[0, wave + 1, rows], send_sem.at[wave % AHEAD, q, 0], recv_sem.at[wave, q, 0], device_id=target))
                copies.append(pltpu.make_async_remote_copy(
                    vbuf.at[0, src + 1, :, rows], vbuf.at[0, wave + 2, :, rows], send_sem.at[wave % AHEAD, q, 1], recv_sem.at[wave, q, 1], device_id=target))
            return copies

        def piece_copies(slot):
            copies = []
            for q in range(4):
                rows = pl.ds(q * quarter, quarter)
                sem = (slot - 1) % AHEAD
                copies.append(pltpu.make_async_remote_copy(
                    xbuf.at[0, slot, rows], xbuf.at[0, slot, rows], send_sem.at[sem, q, 0], recv_sem.at[slot - 1, q, 0], device_id=sibling))
                copies.append(pltpu.make_async_remote_copy(
                    vbuf.at[0, slot + 1, :, rows], vbuf.at[0, slot + 1, :, rows], send_sem.at[sem, q, 1], recv_sem.at[slot - 1, q, 1], device_id=sibling))
            return copies

        def sibling_copies(slot):
            return (
                pltpu.make_async_remote_copy(xbuf.at[0, slot], xbuf.at[1, slot], sib_send.at[0], sib_recv.at[slot, 0], device_id=sibling),
                pltpu.make_async_remote_copy(vbuf.at[0, slot + 1], vbuf.at[1, slot + 1], sib_send.at[1], sib_recv.at[slot, 1], device_id=sibling),
            )

        def y_piece_copy(slot, q, target):
            rows = pl.ds(q * quarter, quarter)
            return pltpu.make_async_remote_copy(
                ybuf.at[0, 1, :, rows], ybuf.at[0, slot + 1, :, rows], ysend_sem.at[slot - 1, q], yrecv_sem.at[slot - 1, q], device_id=target)

        def y_sibling_copy(slot):
            return pltpu.make_async_remote_copy(ybuf.at[0, slot + 1], ybuf.at[1, slot + 1], ysib_send.at[0], ysib_recv.at[slot], device_id=sibling)

        def widen(which, slot, r):
            for lane in range(r * TILE, (r + 1) * TILE, LANES):
                rows = vbuf[which, slot + 1, pl.ds(16, 16), pl.ds(lane, LANES)].astype(F32)
                full = jnp.concatenate([rows, jnp.zeros((LANES - 16, LANES), F32)], axis=0)
                abuf[which, slot, pl.ds(lane, LANES), :] = full.T.astype(BF16)

        def block(buf, which, slot, first):
            gram, part = {}, None
            if first:
                widen(which, slot, 0)
            for u in range(n_u + LAG):
                if first and u + 1 < n_r:
                    widen(which, slot, u + 1)
                if u < n_u:
                    c, r = units[u]
                    rows = pl.ds(r * TILE, TILE)
                    lhs = jnp.concatenate([xbuf[which, slot, rows, :], abuf[which, slot, rows, :]], axis=1)
                    gram[u] = jnp.dot(lhs, wbuf[:, pl.ds(c * TILE, TILE)], preferred_element_type=F32)
                if u >= LAG:
                    c, r = units[u - LAG]
                    tile = jnp.minimum((jnp.exp2(gram.pop(u - LAG) * coef) * scale).astype(BF16), cap)
                    rhs_rows = buf[which, slot + 1, pl.ds(0, 16), pl.ds(r * TILE, TILE)]
                    prod = jnp.dot(jnp.concatenate([rhs_rows] * (PAD // 16), axis=0), tile, preferred_element_type=F32)
                    part = prod if r == 0 else part + prod
                    if r == n_r - 1:
                        total[:, pl.ds(c * TILE, TILE)] += part

        total[...] = jnp.zeros_like(total)
        pl.semaphore_wait(barrier, n_slot)
        for copy in sibling_copies(0):
            copy.start()
        for wave in range(AHEAD):
            for copy in wave_copies(wave):
                copy.start()

        def first_step(slot, carry):
            @pl.when(slot > 0)
            def _():
                for copy in piece_copies(slot):
                    copy.wait()
                for copy in sibling_copies(slot):
                    copy.wait_send()
                    copy.start()

            for wave in range(AHEAD, n_slot - 1):
                @pl.when(slot == wave - AHEAD + 1)
                def _():
                    for copy in wave_copies(wave):
                        copy.start()

            block(vbuf, 0, slot, True)
            for copy in sibling_copies(slot):
                copy.wait_recv()
            block(vbuf, 1, slot, True)
            return carry

        lax.fori_loop(0, n_slot, first_step, 0)
        ybuf[0, 1] = total[pl.ds(0, 16), :].astype(BF16)
        total[...] = jnp.zeros_like(total)
        for copy in sibling_copies(n_slot - 1):
            copy.wait_send()

        y_sibling_copy(0).start()
        for wave, (_, _, prim, sec) in enumerate(WAVES):
            for q in range(4):
                (px, py), (sx, sy) = STEP[q], STEP[(q + 1) % 4]
                y_piece_copy(wave + 1, q, chip_id((prim * px + sec * sx) % side, (prim * py + sec * sy) % side)).start()

        def second_step(slot, carry):
            @pl.when(slot > 0)
            def _():
                for q in range(4):
                    y_piece_copy(slot, q, sibling).wait()
                y_sibling_copy(slot).wait_send()
                y_sibling_copy(slot).start()

            block(ybuf, 0, slot, False)
            y_sibling_copy(slot).wait_recv()
            block(ybuf, 1, slot, False)
            return carry

        lax.fori_loop(0, n_slot, second_step, 0)
        out_ref[...] = total[pl.ds(0, 16), :]
        y_sibling_copy(n_slot - 1).wait_send()

    return kernel, n_slot


def both_passes(n_row, scal, x_loc, vt_loc):
    own, feat = x_loc.shape
    n_col = vt_loc.shape[0]
    kernel, n_slot = make_kernel(n_row, own)
    dma = pltpu.SemaphoreType.DMA
    return pl.pallas_call(
        kernel,
        in_specs=[pl.BlockSpec(memory_space=pltpu.SMEM), pl.BlockSpec(memory_space=pl.ANY), pl.BlockSpec(memory_space=pl.ANY)],
        out_specs=pl.BlockSpec(memory_space=pltpu.VMEM),
        out_shape=jax.ShapeDtypeStruct((n_col, own), F32),
        scratch_shapes=[
            pltpu.VMEM((2, n_slot, own, feat), BF16),
            pltpu.VMEM((2, n_slot, own, feat), BF16),
            pltpu.VMEM((2, n_slot + 1, 32, own), BF16),
            pltpu.VMEM((2, n_slot + 1, n_col, own), BF16),
            pltpu.VMEM((2 * feat, own), BF16),
            pltpu.VMEM((PAD, own), F32),
            dma((2,)),
            dma((AHEAD, 4, 2)),
            dma((n_slot - 1, 4, 2)),
            dma((2,)),
            dma((n_slot, 2)),
            dma((n_slot - 1, 4)),
            dma((n_slot - 1, 4)),
            dma((1,)),
            dma((n_slot,)),
        ],
        compiler_params=pltpu.CompilerParams(collective_id=0, has_side_effects=True, vmem_limit_bytes=64000000),
        name="both_passes",
    )(scal, x_loc, vt_loc)


def solution(mesh):
    def local_program(x_loc, v_loc, length_scale, out_scale):
        ell, scale = length_scale[0], out_scale[0]
        shrink = jnp.where(ell > 2.0**64, 2.0**-70, jnp.where(ell > 2.0**32, 2.0**-32, 1.0)).astype(F32)
        ell = ell * shrink
        scal = jnp.stack([LOG2E / (2.0 * ell * ell), scale, shrink * shrink])
        return both_passes(mesh.shape["row"], scal, x_loc, v_loc.T).T

    row_spec = P(("task", "row"), None)
    return jax.shard_map(local_program, mesh=mesh, in_specs=(row_spec, row_spec, P("task"), P("task")), out_specs=row_spec, check_vma=False)
```

```python
import math

import jax
import jax.numpy as jnp
from jax import lax
from jax.experimental import pallas as pl
from jax.experimental.pallas import tpu as pltpu
from jax.sharding import PartitionSpec as P

BF16 = jnp.bfloat16
F32 = jnp.float32
LOG2E = 1.4426950408889634
TILE = 512
LANES = 128
LAG = 1
PAD = 128
STEP = ((1, 0), (0, 1), (-1, 0), (0, -1))
WAVES = (
    (0, 0, 1, 0),
    (2, 0, -1, 0),
    (3, 0, 0, 1),
    (1, 0, 0, -1),
    (0, 1, 2, 0),
    (3, 1, 1, 1),
    (1, 1, 1, -1),
    (3, 2, -1, 1),
    (1, 2, -1, -1),
    (3, 3, 0, 2),
    (3, 5, 2, 1),
    (1, 5, 2, -1),
    (3, 6, 1, 2),
    (3, 8, -1, 2),
    (3, 11, 2, 2),
)
AHEAD = 4
RING = 3
KEPT_SLOTS = 3


def split3(val):
    high = val.astype(BF16).astype(F32)
    mid = (val - high).astype(BF16).astype(F32)
    low = (val - high) - mid
    return high, mid, low


def make_kernel(n_row, own):
    side = math.isqrt(n_row // 2)
    n_slot = side * side
    quarter = own // 4
    n_c, n_r = own // TILE, own // TILE
    n_far = 2 * (n_slot - KEPT_SLOTS)
    units = [(c, r) for c in range(n_c) for r in range(n_r)]
    n_u = len(units)

    def kernel(
        scal_ref, x_ref, vt_ref, out_ref, store_ref, xbuf, abuf, vbuf, ybuf, wbuf, total, tbuf,
        load_sem, send_sem, recv_sem, sib_send, sib_recv, ysend_sem, yrecv_sem, ysib_send, ysib_recv, spill_sem, fetch_sem,
    ):
        me = lax.axis_index("row")
        core, chip = me % 2, me // 2
        cx, cy = chip % side, chip // side

        def chip_id(dx, dy):
            return {"row": (((cy + dy + side) % side) * side + (cx + dx + side) % side) * 2 + core}

        sibling = {"row": chip * 2 + 1 - core}

        load_x = pltpu.make_async_copy(x_ref, xbuf.at[0, 0], load_sem.at[0])
        load_v = pltpu.make_async_copy(vt_ref, vbuf.at[0, 0, pl.ds(0, 16)], load_sem.at[1])
        load_x.start()
        load_v.start()

        barrier = pltpu.get_barrier_semaphore()
        for k in range(1, n_slot):
            pl.semaphore_signal(barrier, inc=1, device_id=chip_id(k % side, k // side))
        pl.semaphore_signal(barrier, inc=1, device_id=sibling)

        coef, scale, shrink2 = scal_ref[0], scal_ref[1], scal_ref[2]
        cap = jnp.full((TILE, TILE), scale, F32).astype(BF16)
        wbuf[pl.ds(LANES + 16, LANES - 16), :] = jnp.zeros((LANES - 16, own), BF16)

        load_x.wait()
        load_v.wait()
        row_idx = lax.broadcasted_iota(jnp.int32, (16, LANES), 0)
        for r in range(own // LANES):
            x_t = xbuf[0, 0, pl.ds(r * LANES, LANES), :].astype(F32).T
            norm = jnp.sum(x_t * x_t, axis=0, keepdims=True) * shrink2
            parts = [jnp.broadcast_to(p, (16, LANES)) for p in split3(norm)]
            vis = jnp.where(row_idx < 6, 1.0, 0.0)
            mine = jnp.where(row_idx < 3, -1.0, 0.0)
            for i, part in enumerate(parts):
                vis = jnp.where(row_idx == i, part, vis)
                mine = jnp.where(row_idx == i + 3, -part, mine)
            vbuf[0, 0, pl.ds(16, 16), pl.ds(r * LANES, LANES)] = vis.astype(BF16)
            wbuf[pl.ds(0, LANES), pl.ds(r * LANES, LANES)] = (x_t * (2.0 * shrink2)).astype(BF16)
            wbuf[pl.ds(LANES, 16), pl.ds(r * LANES, LANES)] = mine.astype(BF16)

        def wave_copies(wave):
            rel, src, _, _ = WAVES[wave]
            copies = []
            for d in range(4):
                q = (d + rel) % 4
                target = chip_id(*STEP[d])
                rows = pl.ds(q * quarter, quarter)
                copies.append(pltpu.make_async_remote_copy(
                    xbuf.at[0, src, rows], xbuf.at[0, wave + 1, rows], send_sem.at[wave % AHEAD, q, 0], recv_sem.at[wave, q, 0], device_id=target))
                copies.append(pltpu.make_async_remote_copy(
                    vbuf.at[0, src, :, rows], vbuf.at[0, wave + 1, :, rows], send_sem.at[wave % AHEAD, q, 1], recv_sem.at[wave, q, 1], device_id=target))
            return copies

        def piece_copies(slot):
            copies = []
            for q in range(4):
                rows = pl.ds(q * quarter, quarter)
                sem = (slot - 1) % AHEAD
                copies.append(pltpu.make_async_remote_copy(
                    xbuf.at[0, slot, rows], xbuf.at[0, slot, rows], send_sem.at[sem, q, 0], recv_sem.at[slot - 1, q, 0], device_id=sibling))
                copies.append(pltpu.make_async_remote_copy(
                    vbuf.at[0, slot, :, rows], vbuf.at[0, slot, :, rows], send_sem.at[sem, q, 1], recv_sem.at[slot - 1, q, 1], device_id=sibling))
            return copies

        def sibling_copies(slot):
            return (
                pltpu.make_async_remote_copy(xbuf.at[0, slot], xbuf.at[1, slot], sib_send.at[0], sib_recv.at[slot, 0], device_id=sibling),
                pltpu.make_async_remote_copy(vbuf.at[0, slot], vbuf.at[1, slot], sib_send.at[1], sib_recv.at[slot, 1], device_id=sibling),
            )

        def y_piece_copy(slot, q, target):
            rows = pl.ds(q * quarter, quarter)
            return pltpu.make_async_remote_copy(
                ybuf.at[0, 0, :, rows], ybuf.at[0, slot, :, rows], ysend_sem.at[slot - 1, q], yrecv_sem.at[slot - 1, q], device_id=target)

        def y_sibling_copy(slot, chain):
            return pltpu.make_async_remote_copy(ybuf.at[0, slot], ybuf.at[1, slot], ysib_send.at[chain], ysib_recv.at[slot], device_id=sibling)

        def spill(idx):
            return pltpu.make_async_copy(tbuf.at[idx % RING], store_ref.at[idx], spill_sem.at[idx % RING])

        def fetch(idx):
            return pltpu.make_async_copy(store_ref.at[idx], tbuf.at[idx % RING], fetch_sem.at[idx % RING])

        def widen(which, slot, r):
            for lane in range(r * TILE, (r + 1) * TILE, LANES):
                rows = vbuf[which, slot, pl.ds(16, 16), pl.ds(lane, LANES)].astype(F32)
                full = jnp.concatenate([rows, jnp.zeros((LANES - 16, LANES), F32)], axis=0)
                abuf[which, pl.ds(lane, LANES), :] = full.T.astype(BF16)

        def first_block(which, slot):
            idx = 2 * slot + which
            kept = idx // n_far
            place = (idx % RING) * (1 - kept) + (idx - n_far + RING) * kept

            @pl.when((idx >= RING) & (idx < n_far))
            def _():
                spill(idx - RING).wait()

            gram, part = {}, None
            widen(which, slot, 0)
            for u in range(n_u + LAG):
                if u + 1 < n_r:
                    widen(which, slot, u + 1)
                if u < n_u:
                    c, r = units[u]
                    rows = pl.ds(r * TILE, TILE)
                    lhs = jnp.concatenate([xbuf[which, slot, rows, :], abuf[which, rows, :]], axis=1)
                    gram[u] = jnp.dot(lhs, wbuf[:, pl.ds(c * TILE, TILE)], preferred_element_type=F32)
                if u >= LAG:
                    c, r = units[u - LAG]
                    tile = jnp.minimum((jnp.exp2(gram.pop(u - LAG) * coef) * scale).astype(BF16), cap)
                    tbuf[place, pl.ds(r * TILE, TILE), pl.ds(c * TILE, TILE)] = tile
                    v_rows = vbuf[which, slot, pl.ds(0, 16), pl.ds(r * TILE, TILE)]
                    prod = jnp.dot(jnp.concatenate([v_rows] * (PAD // 16), axis=0), tile, preferred_element_type=F32)
                    part = prod if r == 0 else part + prod
                    if r == n_r - 1:
                        total[:, pl.ds(c * TILE, TILE)] += part

            @pl.when(idx < n_far)
            def _():
                spill(idx).start()

        def second_block(place, which, slot):
            for c in range(n_c):
                cols = pl.ds(c * TILE, TILE)
                total[pl.ds(0, 16), cols] += jnp.dot(ybuf[which, slot], tbuf[place, :, cols], preferred_element_type=F32)

        total[...] = jnp.zeros_like(total)
        pl.semaphore_wait(barrier, n_slot)
        for copy in sibling_copies(0):
            copy.start()
        for wave in range(AHEAD):
            for copy in wave_copies(wave):
                copy.start()

        def first_step(slot, carry):
            @pl.when(slot > 0)
            def _():
                for copy in piece_copies(slot):
                    copy.wait()
                for copy in sibling_copies(slot):
                    copy.wait_send()
                    copy.start()

            for wave in range(AHEAD, n_slot - 1):
                @pl.when(slot == wave - AHEAD + 1)
                def _():
                    for copy in wave_copies(wave):
                        copy.start()

            @pl.when(slot == n_slot - KEPT_SLOTS)
            def _():
                for idx in range(RING):
                    spill(n_far - RING + idx).wait()
                for idx in range(RING):
                    fetch(idx).start()

            first_block(0, slot)
            for copy in sibling_copies(slot):
                copy.wait_recv()
            first_block(1, slot)
            return carry

        lax.fori_loop(0, n_slot, first_step, 0)
        ybuf[0, 0] = total[pl.ds(0, 16), :].astype(BF16)
        total[...] = jnp.zeros_like(total)
        for copy in sibling_copies(n_slot - 1):
            copy.wait_send()

        y_sibling_copy(0, 0).start()
        for wave, (_, _, prim, sec) in enumerate(WAVES):
            for q in range(4):
                (px, py), (sx, sy) = STEP[q], STEP[(q + 1) % 4]
                y_piece_copy(wave + 1, q, chip_id((prim * px + sec * sx) % side, (prim * py + sec * sy) % side)).start()

        n_far_slots = n_slot - KEPT_SLOTS

        def far_block(which, slot):
            idx = 2 * slot + which
            fetch(idx).wait()
            second_block(idx % RING, which, slot)

            @pl.when(idx + RING < n_far)
            def _():
                fetch(idx + RING).start()

        def pass_on(slot, chain):
            for q in range(4):
                y_piece_copy(slot, q, sibling).wait()
            y_sibling_copy(slot, chain).start()

        def second_step(slot, carry):
            @pl.when(slot > 0)
            def _():
                y_sibling_copy(slot, 0).wait_send()
                pass_on(slot, 0)

            far_block(0, slot)
            y_sibling_copy(slot, 0).wait_recv()
            far_block(1, slot)
            near = slot - (n_far_slots - 2 * KEPT_SLOTS)
            near_slot = n_far_slots + near // 2

            @pl.when((near >= 0) & (near % 2 == 0))
            def _():
                pass_on(near_slot, 1)
                second_block(RING + near, 0, near_slot)

            @pl.when((near >= 0) & (near % 2 == 1))
            def _():
                y_sibling_copy(near_slot, 1).wait_send()
                y_sibling_copy(near_slot, 1).wait_recv()
                second_block(RING + near, 1, near_slot)

            return carry

        lax.fori_loop(0, n_far_slots, second_step, 0)
        out_ref[...] = total[pl.ds(0, 16), :]
        y_sibling_copy(n_far_slots - 1, 0).wait_send()

    return kernel, n_slot


def both_passes(n_row, scal, x_loc, vt_loc):
    own, feat = x_loc.shape
    n_col = vt_loc.shape[0]
    kernel, n_slot = make_kernel(n_row, own)
    dma = pltpu.SemaphoreType.DMA
    return pl.pallas_call(
        kernel,
        in_specs=[pl.BlockSpec(memory_space=pltpu.SMEM), pl.BlockSpec(memory_space=pl.ANY), pl.BlockSpec(memory_space=pl.ANY)],
        out_specs=[pl.BlockSpec(memory_space=pltpu.VMEM), pl.BlockSpec(memory_space=pl.ANY)],
        out_shape=[jax.ShapeDtypeStruct((n_col, own), F32), jax.ShapeDtypeStruct((2 * (n_slot - KEPT_SLOTS), own, own), BF16)],
        scratch_shapes=[
            pltpu.VMEM((2, n_slot, own, feat), BF16),
            pltpu.VMEM((2, own, feat), BF16),
            pltpu.VMEM((2, n_slot, 32, own), BF16),
            pltpu.VMEM((2, n_slot, n_col, own), BF16),
            pltpu.VMEM((2 * feat, own), BF16),
            pltpu.VMEM((PAD, own), F32),
            pltpu.VMEM((RING + 2 * KEPT_SLOTS, own, own), BF16),
            dma((2,)),
            dma((AHEAD, 4, 2)),
            dma((n_slot - 1, 4, 2)),
            dma((2,)),
            dma((n_slot, 2)),
            dma((n_slot - 1, 4)),
            dma((n_slot - 1, 4)),
            dma((2,)),
            dma((n_slot,)),
            dma((RING,)),
            dma((RING,)),
        ],
        compiler_params=pltpu.CompilerParams(collective_id=0, has_side_effects=True, vmem_limit_bytes=67000000),
        name="both_passes",
    )(scal, x_loc, vt_loc)[0]


def solution(mesh):
    def local_program(x_loc, v_loc, length_scale, out_scale):
        ell, scale = length_scale[0], out_scale[0]
        shrink = jnp.where(ell > 2.0**64, 2.0**-70, jnp.where(ell > 2.0**32, 2.0**-32, 1.0)).astype(F32)
        ell = ell * shrink
        scal = jnp.stack([LOG2E / (2.0 * ell * ell), scale, shrink * shrink])
        return both_passes(mesh.shape["row"], scal, x_loc, v_loc.T).T

    row_spec = P(("task", "row"), None)
    return jax.shard_map(local_program, mesh=mesh, in_specs=(row_spec, row_spec, P("task"), P("task")), out_specs=row_spec, check_vma=False)
```

```python
import math

import jax
import jax.numpy as jnp
from jax import lax
from jax.experimental import pallas as pl
from jax.experimental.pallas import tpu as pltpu
from jax.sharding import PartitionSpec as P

BF16 = jnp.bfloat16
F32 = jnp.float32
LOG2E = 1.4426950408889634
TILE = 512
LANES = 128
LAG = 1
PAD = 96
STEP = ((1, 0), (0, 1), (-1, 0), (0, -1))
WAVES = (
    (0, 0, 1, 0),
    (2, 0, -1, 0),
    (3, 0, 0, 1),
    (1, 0, 0, -1),
    (0, 1, 2, 0),
    (3, 1, 1, 1),
    (1, 1, 1, -1),
    (3, 2, -1, 1),
    (1, 2, -1, -1),
    (3, 3, 0, 2),
    (3, 5, 2, 1),
    (1, 5, 2, -1),
    (3, 6, 1, 2),
    (3, 8, -1, 2),
    (3, 11, 2, 2),
)
AHEAD = 4
RING = 3
KEPT_SLOTS = 3


def split3(val):
    high = val.astype(BF16).astype(F32)
    mid = (val - high).astype(BF16).astype(F32)
    low = (val - high) - mid
    return high, mid, low


def make_kernel(n_row, own):
    side = math.isqrt(n_row // 2)
    n_slot = side * side
    quarter = own // 4
    n_c, n_r = own // TILE, own // TILE
    n_far = 2 * (n_slot - KEPT_SLOTS)
    units = [(c, r) for c in range(n_c) for r in range(n_r)]
    n_u = len(units)

    def kernel(
        scal_ref, x_ref, vt_ref, out_ref, store_ref, xbuf, abuf, vbuf, ybuf, wbuf, total, tbuf,
        load_sem, send_sem, recv_sem, sib_send, sib_recv, ysend_sem, yrecv_sem, ysib_send, ysib_recv, spill_sem, fetch_sem,
    ):
        me = lax.axis_index("row")
        core, chip = me % 2, me // 2
        cx, cy = chip % side, chip // side

        def chip_id(dx, dy):
            return {"row": (((cy + dy + side) % side) * side + (cx + dx + side) % side) * 2 + core}

        sibling = {"row": chip * 2 + 1 - core}

        load_x = pltpu.make_async_copy(x_ref, xbuf.at[0, 0], load_sem.at[0])
        load_v = pltpu.make_async_copy(vt_ref, vbuf.at[0, 0, pl.ds(0, 16)], load_sem.at[1])
        load_x.start()
        load_v.start()

        barrier = pltpu.get_barrier_semaphore()
        for k in range(1, n_slot):
            pl.semaphore_signal(barrier, inc=1, device_id=chip_id(k % side, k // side))
        pl.semaphore_signal(barrier, inc=1, device_id=sibling)

        coef, scale, shrink2 = scal_ref[0], scal_ref[1], scal_ref[2]
        cap = jnp.full((TILE, TILE), scale, F32).astype(BF16)
        wbuf[pl.ds(LANES + 16, LANES - 16), :] = jnp.zeros((LANES - 16, own), BF16)

        load_x.wait()
        load_v.wait()
        row_idx = lax.broadcasted_iota(jnp.int32, (16, LANES), 0)
        for r in range(own // LANES):
            x_t = xbuf[0, 0, pl.ds(r * LANES, LANES), :].astype(F32).T
            norm = jnp.sum(x_t * x_t, axis=0, keepdims=True) * shrink2
            parts = [jnp.broadcast_to(p, (16, LANES)) for p in split3(norm)]
            vis = jnp.where(row_idx < 6, 1.0, 0.0)
            mine = jnp.where(row_idx < 3, -1.0, 0.0)
            for i, part in enumerate(parts):
                vis = jnp.where(row_idx == i, part, vis)
                mine = jnp.where(row_idx == i + 3, -part, mine)
            vbuf[0, 0, pl.ds(16, 16), pl.ds(r * LANES, LANES)] = vis.astype(BF16)
            wbuf[pl.ds(0, LANES), pl.ds(r * LANES, LANES)] = (x_t * (2.0 * shrink2)).astype(BF16)
            wbuf[pl.ds(LANES, 16), pl.ds(r * LANES, LANES)] = mine.astype(BF16)

        def wave_copies(wave):
            rel, src, _, _ = WAVES[wave]
            copies = []
            for d in range(4):
                q = (d + rel) % 4
                target = chip_id(*STEP[d])
                rows = pl.ds(q * quarter, quarter)
                copies.append(pltpu.make_async_remote_copy(
                    xbuf.at[0, src, rows], xbuf.at[0, wave + 1, rows], send_sem.at[wave % AHEAD, q, 0], recv_sem.at[wave, q, 0], device_id=target))
                copies.append(pltpu.make_async_remote_copy(
                    vbuf.at[0, src, :, rows], vbuf.at[0, wave + 1, :, rows], send_sem.at[wave % AHEAD, q, 1], recv_sem.at[wave, q, 1], device_id=target))
            return copies

        def piece_copies(slot):
            copies = []
            for q in range(4):
                rows = pl.ds(q * quarter, quarter)
                sem = (slot - 1) % AHEAD
                copies.append(pltpu.make_async_remote_copy(
                    xbuf.at[0, slot, rows], xbuf.at[0, slot, rows], send_sem.at[sem, q, 0], recv_sem.at[slot - 1, q, 0], device_id=sibling))
                copies.append(pltpu.make_async_remote_copy(
                    vbuf.at[0, slot, :, rows], vbuf.at[0, slot, :, rows], send_sem.at[sem, q, 1], recv_sem.at[slot - 1, q, 1], device_id=sibling))
            return copies

        def sibling_copies(slot):
            return (
                pltpu.make_async_remote_copy(xbuf.at[0, slot], xbuf.at[1, slot], sib_send.at[0], sib_recv.at[slot, 0], device_id=sibling),
                pltpu.make_async_remote_copy(vbuf.at[0, slot], vbuf.at[1, slot], sib_send.at[1], sib_recv.at[slot, 1], device_id=sibling),
            )

        def y_piece_copy(slot, q, target):
            rows = pl.ds(q * quarter, quarter)
            return pltpu.make_async_remote_copy(
                ybuf.at[0, 0, :, rows], ybuf.at[0, slot, :, rows], ysend_sem.at[slot - 1, q], yrecv_sem.at[slot - 1, q], device_id=target)

        def y_sibling_copy(slot, chain):
            return pltpu.make_async_remote_copy(ybuf.at[0, slot], ybuf.at[1, slot], ysib_send.at[chain], ysib_recv.at[slot], device_id=sibling)

        def spill(idx):
            return pltpu.make_async_copy(tbuf.at[idx % RING], store_ref.at[idx], spill_sem.at[idx % RING])

        def fetch(idx):
            return pltpu.make_async_copy(store_ref.at[idx], tbuf.at[idx % RING], fetch_sem.at[idx % RING])

        def widen(which, slot, r):
            for lane in range(r * TILE, (r + 1) * TILE, LANES):
                rows = vbuf[which, slot, pl.ds(16, 16), pl.ds(lane, LANES)].astype(F32)
                full = jnp.concatenate([rows, jnp.zeros((LANES - 16, LANES), F32)], axis=0)
                abuf[which, pl.ds(lane, LANES), :] = full.T.astype(BF16)

        def first_block(which, slot):
            idx = 2 * slot + which
            kept = idx // n_far
            place = (idx % RING) * (1 - kept) + (idx - n_far + RING) * kept

            @pl.when((idx >= RING) & (idx < n_far))
            def _():
                spill(idx - RING).wait()

            gram, part = {}, None
            widen(which, slot, 0)
            for u in range(n_u + LAG):
                if u + 1 < n_r:
                    widen(which, slot, u + 1)
                if u < n_u:
                    c, r = units[u]
                    rows = pl.ds(r * TILE, TILE)
                    lhs = jnp.concatenate([xbuf[which, slot, rows, :], abuf[which, rows, :]], axis=1)
                    gram[u] = jnp.dot(lhs, wbuf[:, pl.ds(c * TILE, TILE)], preferred_element_type=F32)
                if u >= LAG:
                    c, r = units[u - LAG]
                    tile = jnp.minimum((jnp.exp2(gram.pop(u - LAG) * coef) * scale).astype(BF16), cap)
                    tbuf[place, pl.ds(r * TILE, TILE), pl.ds(c * TILE, TILE)] = tile
                    v_rows = vbuf[which, slot, pl.ds(0, 16), pl.ds(r * TILE, TILE)]
                    prod = jnp.dot(jnp.concatenate([v_rows] * (PAD // 16), axis=0), tile, preferred_element_type=F32)
                    part = prod if r == 0 else part + prod
                    if r == n_r - 1:
                        total[:, pl.ds(c * TILE, TILE)] += part

            @pl.when(idx < n_far)
            def _():
                spill(idx).start()

        def second_block(place, which, slot):
            for c in range(n_c):
                cols = pl.ds(c * TILE, TILE)
                total[pl.ds(0, 16), cols] += jnp.dot(ybuf[which, slot], tbuf[place, :, cols], preferred_element_type=F32)

        total[...] = jnp.zeros_like(total)
        pl.semaphore_wait(barrier, n_slot)
        for copy in sibling_copies(0):
            copy.start()
        for wave in range(AHEAD):
            for copy in wave_copies(wave):
                copy.start()

        def first_step(slot, carry):
            @pl.when(slot > 0)
            def _():
                for copy in piece_copies(slot):
                    copy.wait()
                for copy in sibling_copies(slot):
                    copy.wait_send()
                    copy.start()

            for wave in range(AHEAD, n_slot - 1):
                @pl.when(slot == wave - AHEAD + 1)
                def _():
                    for copy in wave_copies(wave):
                        copy.start()

            @pl.when(slot == n_slot - KEPT_SLOTS)
            def _():
                for idx in range(RING):
                    spill(n_far - RING + idx).wait()
                for idx in range(RING):
                    fetch(idx).start()

            first_block(0, slot)
            for copy in sibling_copies(slot):
                copy.wait_recv()
            first_block(1, slot)
            return carry

        lax.fori_loop(0, n_slot, first_step, 0)
        ybuf[0, 0] = total[pl.ds(0, 16), :].astype(BF16)
        total[...] = jnp.zeros_like(total)
        for copy in sibling_copies(n_slot - 1):
            copy.wait_send()

        y_sibling_copy(0, 0).start()
        for wave, (_, _, prim, sec) in enumerate(WAVES):
            for q in range(4):
                (px, py), (sx, sy) = STEP[q], STEP[(q + 1) % 4]
                y_piece_copy(wave + 1, q, chip_id((prim * px + sec * sx) % side, (prim * py + sec * sy) % side)).start()

        n_far_slots = n_slot - KEPT_SLOTS

        def far_block(which, slot):
            idx = 2 * slot + which
            fetch(idx).wait()
            second_block(idx % RING, which, slot)

            @pl.when(idx + RING < n_far)
            def _():
                fetch(idx + RING).start()

        def pass_on(slot, chain):
            for q in range(4):
                y_piece_copy(slot, q, sibling).wait()
            y_sibling_copy(slot, chain).start()

        def second_step(slot, carry):
            @pl.when(slot > 0)
            def _():
                y_sibling_copy(slot, 0).wait_send()
                pass_on(slot, 0)

            far_block(0, slot)
            y_sibling_copy(slot, 0).wait_recv()
            far_block(1, slot)
            near = slot - (n_far_slots - 2 * KEPT_SLOTS)
            near_slot = n_far_slots + near // 2

            @pl.when((near >= 0) & (near % 2 == 0))
            def _():
                pass_on(near_slot, 1)
                second_block(RING + near, 0, near_slot)

            @pl.when((near >= 0) & (near % 2 == 1))
            def _():
                y_sibling_copy(near_slot, 1).wait_send()
                y_sibling_copy(near_slot, 1).wait_recv()
                second_block(RING + near, 1, near_slot)

            return carry

        lax.fori_loop(0, n_far_slots, second_step, 0)
        out_ref[...] = total[pl.ds(0, 16), :]
        y_sibling_copy(n_far_slots - 1, 0).wait_send()

    return kernel, n_slot


def both_passes(n_row, scal, x_loc, vt_loc):
    own, feat = x_loc.shape
    n_col = vt_loc.shape[0]
    kernel, n_slot = make_kernel(n_row, own)
    dma = pltpu.SemaphoreType.DMA
    return pl.pallas_call(
        kernel,
        in_specs=[pl.BlockSpec(memory_space=pltpu.SMEM), pl.BlockSpec(memory_space=pl.ANY), pl.BlockSpec(memory_space=pl.ANY)],
        out_specs=[pl.BlockSpec(memory_space=pltpu.VMEM), pl.BlockSpec(memory_space=pl.ANY)],
        out_shape=[jax.ShapeDtypeStruct((n_col, own), F32), jax.ShapeDtypeStruct((2 * (n_slot - KEPT_SLOTS), own, own), BF16)],
        scratch_shapes=[
            pltpu.VMEM((2, n_slot, own, feat), BF16),
            pltpu.VMEM((2, own, feat), BF16),
            pltpu.VMEM((2, n_slot, 32, own), BF16),
            pltpu.VMEM((2, n_slot, n_col, own), BF16),
            pltpu.VMEM((2 * feat, own), BF16),
            pltpu.VMEM((PAD, own), F32),
            pltpu.VMEM((RING + 2 * KEPT_SLOTS, own, own), BF16),
            dma((2,)),
            dma((AHEAD, 4, 2)),
            dma((n_slot - 1, 4, 2)),
            dma((2,)),
            dma((n_slot, 2)),
            dma((n_slot - 1, 4)),
            dma((n_slot - 1, 4)),
            dma((2,)),
            dma((n_slot,)),
            dma((RING,)),
            dma((RING,)),
        ],
        compiler_params=pltpu.CompilerParams(collective_id=0, has_side_effects=True, vmem_limit_bytes=67000000),
        name="both_passes",
    )(scal, x_loc, vt_loc)[0]


def solution(mesh):
    def local_program(x_loc, v_loc, length_scale, out_scale):
        ell, scale = length_scale[0], out_scale[0]
        shrink = jnp.where(ell > 2.0**64, 2.0**-70, jnp.where(ell > 2.0**32, 2.0**-32, 1.0)).astype(F32)
        ell = ell * shrink
        scal = jnp.stack([LOG2E / (2.0 * ell * ell), scale, shrink * shrink])
        return both_passes(mesh.shape["row"], scal, x_loc, v_loc.T).T

    row_spec = P(("task", "row"), None)
    return jax.shard_map(local_program, mesh=mesh, in_specs=(row_spec, row_spec, P("task"), P("task")), out_specs=row_spec, check_vma=False)
```

```python
import math

import jax
import jax.numpy as jnp
from jax import lax
from jax.experimental import pallas as pl
from jax.experimental.pallas import tpu as pltpu
from jax.sharding import PartitionSpec as P

BF16 = jnp.bfloat16
F32 = jnp.float32
LOG2E = 1.4426950408889634
TILE = 512
LANES = 128
LAG = 1
PAD = 96
STEP = ((1, 0), (0, 1), (-1, 0), (0, -1))
WAVES = (
    (0, 0, 1, 0),
    (2, 0, -1, 0),
    (3, 0, 0, 1),
    (1, 0, 0, -1),
    (0, 1, 2, 0),
    (3, 1, 1, 1),
    (1, 1, 1, -1),
    (3, 2, -1, 1),
    (1, 2, -1, -1),
    (3, 3, 0, 2),
    (3, 5, 2, 1),
    (1, 5, 2, -1),
    (3, 6, 1, 2),
    (3, 8, -1, 2),
    (3, 11, 2, 2),
)
AHEAD = 4
RING = 3
KEPT_SLOTS = 3
REDO_SLOTS = 2


def split3(val):
    high = val.astype(BF16).astype(F32)
    mid = (val - high).astype(BF16).astype(F32)
    low = (val - high) - mid
    return high, mid, low


def make_kernel(n_row, own):
    side = math.isqrt(n_row // 2)
    n_slot = side * side
    quarter = own // 4
    n_c, n_r = own // TILE, own // TILE
    n_far_slots = n_slot - KEPT_SLOTS - REDO_SLOTS
    n_far, n_ring = 2 * n_far_slots, 2 * (n_slot - KEPT_SLOTS)
    units = [(c, r) for c in range(n_c) for r in range(n_r)]
    n_u = len(units)

    def kernel(
        scal_ref, x_ref, vt_ref, out_ref, store_ref, xbuf, abuf, vbuf, ybuf, wbuf, total, tbuf,
        load_sem, send_sem, recv_sem, sib_send, sib_recv, ysend_sem, yrecv_sem, ysib_send, ysib_recv, spill_sem, fetch_sem,
    ):
        me = lax.axis_index("row")
        core, chip = me % 2, me // 2
        cx, cy = chip % side, chip // side

        def chip_id(dx, dy):
            return {"row": (((cy + dy + side) % side) * side + (cx + dx + side) % side) * 2 + core}

        sibling = {"row": chip * 2 + 1 - core}

        load_x = pltpu.make_async_copy(x_ref, xbuf.at[0, 0], load_sem.at[0])
        load_v = pltpu.make_async_copy(vt_ref, vbuf.at[0, 0, pl.ds(0, 16)], load_sem.at[1])
        load_x.start()
        load_v.start()

        barrier = pltpu.get_barrier_semaphore()
        for k in range(1, n_slot):
            pl.semaphore_signal(barrier, inc=1, device_id=chip_id(k % side, k // side))
        pl.semaphore_signal(barrier, inc=1, device_id=sibling)

        coef, scale, shrink2 = scal_ref[0], scal_ref[1], scal_ref[2]
        cap = jnp.full((TILE, TILE), scale, F32).astype(BF16)
        wbuf[pl.ds(LANES + 16, LANES - 16), :] = jnp.zeros((LANES - 16, own), BF16)

        load_x.wait()
        load_v.wait()
        row_idx = lax.broadcasted_iota(jnp.int32, (16, LANES), 0)
        for r in range(own // LANES):
            x_t = xbuf[0, 0, pl.ds(r * LANES, LANES), :].astype(F32).T
            norm = jnp.sum(x_t * x_t, axis=0, keepdims=True) * shrink2
            parts = [jnp.broadcast_to(p, (16, LANES)) for p in split3(norm)]
            vis = jnp.where(row_idx < 6, 1.0, 0.0)
            mine = jnp.where(row_idx < 3, -1.0, 0.0)
            for i, part in enumerate(parts):
                vis = jnp.where(row_idx == i, part, vis)
                mine = jnp.where(row_idx == i + 3, -part, mine)
            vbuf[0, 0, pl.ds(16, 16), pl.ds(r * LANES, LANES)] = vis.astype(BF16)
            wbuf[pl.ds(0, LANES), pl.ds(r * LANES, LANES)] = (x_t * (2.0 * shrink2)).astype(BF16)
            wbuf[pl.ds(LANES, 16), pl.ds(r * LANES, LANES)] = mine.astype(BF16)

        def wave_copies(wave):
            rel, src, _, _ = WAVES[wave]
            copies = []
            for d in range(4):
                q = (d + rel) % 4
                target = chip_id(*STEP[d])
                rows = pl.ds(q * quarter, quarter)
                copies.append(pltpu.make_async_remote_copy(
                    xbuf.at[0, src, rows], xbuf.at[0, wave + 1, rows], send_sem.at[wave % AHEAD, q, 0], recv_sem.at[wave, q, 0], device_id=target))
                copies.append(pltpu.make_async_remote_copy(
                    vbuf.at[0, src, :, rows], vbuf.at[0, wave + 1, :, rows], send_sem.at[wave % AHEAD, q, 1], recv_sem.at[wave, q, 1], device_id=target))
            return copies

        def piece_copies(slot):
            copies = []
            for q in range(4):
                rows = pl.ds(q * quarter, quarter)
                sem = (slot - 1) % AHEAD
                copies.append(pltpu.make_async_remote_copy(
                    xbuf.at[0, slot, rows], xbuf.at[0, slot, rows], send_sem.at[sem, q, 0], recv_sem.at[slot - 1, q, 0], device_id=sibling))
                copies.append(pltpu.make_async_remote_copy(
                    vbuf.at[0, slot, :, rows], vbuf.at[0, slot, :, rows], send_sem.at[sem, q, 1], recv_sem.at[slot - 1, q, 1], device_id=sibling))
            return copies

        def sibling_copies(slot):
            return (
                pltpu.make_async_remote_copy(xbuf.at[0, slot], xbuf.at[1, slot], sib_send.at[0], sib_recv.at[slot, 0], device_id=sibling),
                pltpu.make_async_remote_copy(vbuf.at[0, slot], vbuf.at[1, slot], sib_send.at[1], sib_recv.at[slot, 1], device_id=sibling),
            )

        def y_piece_copy(slot, q, target):
            rows = pl.ds(q * quarter, quarter)
            return pltpu.make_async_remote_copy(
                ybuf.at[0, 0, :, rows], ybuf.at[0, slot, :, rows], ysend_sem.at[slot - 1, q], yrecv_sem.at[slot - 1, q], device_id=target)

        def y_sibling_copy(slot, chain):
            return pltpu.make_async_remote_copy(ybuf.at[0, slot], ybuf.at[1, slot], ysib_send.at[chain], ysib_recv.at[slot], device_id=sibling)

        def spill(idx):
            return pltpu.make_async_copy(tbuf.at[idx % RING], store_ref.at[idx], spill_sem.at[idx % RING])

        def fetch(idx):
            return pltpu.make_async_copy(store_ref.at[idx], tbuf.at[idx % RING], fetch_sem.at[idx % RING])

        def widen(which, slot, r):
            for lane in range(r * TILE, (r + 1) * TILE, LANES):
                rows = vbuf[which, slot, pl.ds(16, 16), pl.ds(lane, LANES)].astype(F32)
                full = jnp.concatenate([rows, jnp.zeros((LANES - 16, LANES), F32)], axis=0)
                abuf[which, pl.ds(lane, LANES), :] = full.T.astype(BF16)

        def tiles(buf, which, slot, place):
            gram, part = {}, None
            widen(which, slot, 0)
            for u in range(n_u + LAG):
                if u + 1 < n_r:
                    widen(which, slot, u + 1)
                if u < n_u:
                    c, r = units[u]
                    rows = pl.ds(r * TILE, TILE)
                    lhs = jnp.concatenate([xbuf[which, slot, rows, :], abuf[which, rows, :]], axis=1)
                    gram[u] = jnp.dot(lhs, wbuf[:, pl.ds(c * TILE, TILE)], preferred_element_type=F32)
                if u >= LAG:
                    c, r = units[u - LAG]
                    tile = jnp.minimum((jnp.exp2(gram.pop(u - LAG) * coef) * scale).astype(BF16), cap)
                    if place is not None:
                        tbuf[place, pl.ds(r * TILE, TILE), pl.ds(c * TILE, TILE)] = tile
                    v_rows = buf[which, slot, pl.ds(0, 16), pl.ds(r * TILE, TILE)]
                    prod = jnp.dot(jnp.concatenate([v_rows] * (PAD // 16), axis=0), tile, preferred_element_type=F32)
                    part = prod if r == 0 else part + prod
                    if r == n_r - 1:
                        total[:, pl.ds(c * TILE, TILE)] += part

        def first_block(which, slot):
            idx = 2 * slot + which
            kept = idx // n_ring
            place = (idx % RING) * (1 - kept) + (idx - n_ring + RING) * kept

            @pl.when((idx >= RING) & (idx < n_far + RING))
            def _():
                spill(idx - RING).wait()

            tiles(vbuf, which, slot, place)

            @pl.when(idx < n_far)
            def _():
                spill(idx).start()

        def second_block(place, which, slot):
            for c in range(n_c):
                cols = pl.ds(c * TILE, TILE)
                total[pl.ds(0, 16), cols] += jnp.dot(ybuf[which, slot], tbuf[place, :, cols], preferred_element_type=F32)

        total[...] = jnp.zeros_like(total)
        pl.semaphore_wait(barrier, n_slot)
        for copy in sibling_copies(0):
            copy.start()
        for wave in range(AHEAD):
            for copy in wave_copies(wave):
                copy.start()

        def first_step(slot, carry):
            @pl.when(slot > 0)
            def _():
                for copy in piece_copies(slot):
                    copy.wait()
                for copy in sibling_copies(slot):
                    copy.wait_send()
                    copy.start()

            for wave in range(AHEAD, n_slot - 1):
                @pl.when(slot == wave - AHEAD + 1)
                def _():
                    for copy in wave_copies(wave):
                        copy.start()

            @pl.when(slot == n_slot - KEPT_SLOTS)
            def _():
                for idx in range(RING):
                    fetch(idx).start()

            first_block(0, slot)
            for copy in sibling_copies(slot):
                copy.wait_recv()
            first_block(1, slot)
            return carry

        lax.fori_loop(0, n_slot, first_step, 0)
        ybuf[0, 0] = total[pl.ds(0, 16), :].astype(BF16)
        total[...] = jnp.zeros_like(total)
        for copy in sibling_copies(n_slot - 1):
            copy.wait_send()

        y_sibling_copy(0, 0).start()
        for wave, (_, _, prim, sec) in enumerate(WAVES):
            for q in range(4):
                (px, py), (sx, sy) = STEP[q], STEP[(q + 1) % 4]
                y_piece_copy(wave + 1, q, chip_id((prim * px + sec * sx) % side, (prim * py + sec * sy) % side)).start()


        def far_block(which, slot):
            idx = 2 * slot + which
            fetch(idx).wait()
            second_block(idx % RING, which, slot)

            @pl.when(idx + RING < n_far)
            def _():
                fetch(idx + RING).start()

        def pass_on(slot, chain):
            for q in range(4):
                y_piece_copy(slot, q, sibling).wait()
            y_sibling_copy(slot, chain).start()

        def second_step(slot, carry):
            @pl.when(slot > 0)
            def _():
                y_sibling_copy(slot, 0).wait_send()
                pass_on(slot, 0)

            far_block(0, slot)
            y_sibling_copy(slot, 0).wait_recv()
            far_block(1, slot)
            redo = (slot - 3) // 2
            redo_slot = n_far_slots + redo // 2

            for half in (0, 1):
                @pl.when((slot >= 3) & (slot % 2 == 1) & (redo < 2 * REDO_SLOTS) & (redo % 2 == half))
                def _():
                    if half == 0:
                        @pl.when(redo > 0)
                        def _():
                            y_sibling_copy(redo_slot, 2).wait_send()
                        pass_on(redo_slot, 2)
                    else:
                        y_sibling_copy(redo_slot, 2).wait_recv()
                    tiles(ybuf, half, redo_slot, None)

            near = slot - (n_far_slots - 2 * KEPT_SLOTS)
            near_slot = n_far_slots + REDO_SLOTS + near // 2

            @pl.when((near >= 0) & (near % 2 == 0))
            def _():
                pass_on(near_slot, 1)
                second_block(RING + near, 0, near_slot)

            @pl.when((near >= 0) & (near % 2 == 1))
            def _():
                y_sibling_copy(near_slot, 1).wait_send()
                y_sibling_copy(near_slot, 1).wait_recv()
                second_block(RING + near, 1, near_slot)

            return carry

        lax.fori_loop(0, n_far_slots, second_step, 0)
        out_ref[...] = total[pl.ds(0, 16), :]
        y_sibling_copy(n_far_slots - 1, 0).wait_send()
        y_sibling_copy(n_far_slots + REDO_SLOTS - 1, 2).wait_send()

    return kernel, n_slot


def both_passes(n_row, scal, x_loc, vt_loc):
    own, feat = x_loc.shape
    n_col = vt_loc.shape[0]
    kernel, n_slot = make_kernel(n_row, own)
    dma = pltpu.SemaphoreType.DMA
    return pl.pallas_call(
        kernel,
        in_specs=[pl.BlockSpec(memory_space=pltpu.SMEM), pl.BlockSpec(memory_space=pl.ANY), pl.BlockSpec(memory_space=pl.ANY)],
        out_specs=[pl.BlockSpec(memory_space=pltpu.VMEM), pl.BlockSpec(memory_space=pl.ANY)],
        out_shape=[jax.ShapeDtypeStruct((n_col, own), F32), jax.ShapeDtypeStruct((2 * (n_slot - KEPT_SLOTS - REDO_SLOTS), own, own), BF16)],
        scratch_shapes=[
            pltpu.VMEM((2, n_slot, own, feat), BF16),
            pltpu.VMEM((2, own, feat), BF16),
            pltpu.VMEM((2, n_slot, 32, own), BF16),
            pltpu.VMEM((2, n_slot, n_col, own), BF16),
            pltpu.VMEM((2 * feat, own), BF16),
            pltpu.VMEM((PAD, own), F32),
            pltpu.VMEM((RING + 2 * KEPT_SLOTS, own, own), BF16),
            dma((2,)),
            dma((AHEAD, 4, 2)),
            dma((n_slot - 1, 4, 2)),
            dma((2,)),
            dma((n_slot, 2)),
            dma((n_slot - 1, 4)),
            dma((n_slot - 1, 4)),
            dma((3,)),
            dma((n_slot,)),
            dma((RING,)),
            dma((RING,)),
        ],
        compiler_params=pltpu.CompilerParams(collective_id=0, has_side_effects=True, vmem_limit_bytes=67000000),
        name="both_passes",
    )(scal, x_loc, vt_loc)[0]


def solution(mesh):
    def local_program(x_loc, v_loc, length_scale, out_scale):
        ell, scale = length_scale[0], out_scale[0]
        shrink = jnp.where(ell > 2.0**64, 2.0**-70, jnp.where(ell > 2.0**32, 2.0**-32, 1.0)).astype(F32)
        ell = ell * shrink
        scal = jnp.stack([LOG2E / (2.0 * ell * ell), scale, shrink * shrink])
        return both_passes(mesh.shape["row"], scal, x_loc, v_loc.T).T

    row_spec = P(("task", "row"), None)
    return jax.shard_map(local_program, mesh=mesh, in_specs=(row_spec, row_spec, P("task"), P("task")), out_specs=row_spec, check_vma=False)
```

```python
import math

import jax
import jax.numpy as jnp
from jax import lax
from jax.experimental import pallas as pl
from jax.experimental.pallas import tpu as pltpu
from jax.sharding import PartitionSpec as P

BF16 = jnp.bfloat16
F32 = jnp.float32
LOG2E = 1.4426950408889634
TILE = 512
LANES = 128
LAG = 1
PAD = 96
STEP = ((1, 0), (0, 1), (-1, 0), (0, -1))
WAVES = (
    (0, 0, 1, 0),
    (2, 0, -1, 0),
    (3, 0, 0, 1),
    (1, 0, 0, -1),
    (0, 1, 2, 0),
    (3, 1, 1, 1),
    (1, 1, 1, -1),
    (3, 2, -1, 1),
    (1, 2, -1, -1),
    (3, 3, 0, 2),
    (3, 5, 2, 1),
    (1, 5, 2, -1),
    (3, 6, 1, 2),
    (3, 8, -1, 2),
    (3, 11, 2, 2),
)
AHEAD = 4
RING = 3
KEPT_SLOTS = 3


def split3(val):
    high = val.astype(BF16).astype(F32)
    mid = (val - high).astype(BF16).astype(F32)
    low = (val - high) - mid
    return high, mid, low


def make_kernel(n_row, own):
    side = math.isqrt(n_row // 2)
    n_slot = side * side
    quarter = own // 4
    n_c, n_r = own // TILE, own // TILE
    n_far = 2 * (n_slot - KEPT_SLOTS)
    units = [(c, r) for c in range(n_c) for r in range(n_r)]
    n_u = len(units)

    def kernel(
        scal_ref, x_ref, vt_ref, out_ref, store_ref, xbuf, abuf, vbuf, ybuf, wbuf, total, tbuf,
        load_sem, send_sem, recv_sem, sib_send, sib_recv, ysend_sem, yrecv_sem, ysib_send, ysib_recv, spill_sem, fetch_sem,
    ):
        me = lax.axis_index("row")
        core, chip = me % 2, me // 2
        cx, cy = chip % side, chip // side

        def chip_id(dx, dy):
            return {"row": (((cy + dy + side) % side) * side + (cx + dx + side) % side) * 2 + core}

        sibling = {"row": chip * 2 + 1 - core}

        load_x = pltpu.make_async_copy(x_ref, xbuf.at[0, 0], load_sem.at[0])
        load_v = pltpu.make_async_copy(vt_ref, vbuf.at[0, 0, pl.ds(0, 16)], load_sem.at[1])
        load_x.start()
        load_v.start()

        barrier = pltpu.get_barrier_semaphore()
        for k in range(1, n_slot):
            pl.semaphore_signal(barrier, inc=1, device_id=chip_id(k % side, k // side))
        pl.semaphore_signal(barrier, inc=1, device_id=sibling)

        coef, scale, shrink2 = scal_ref[0], scal_ref[1], scal_ref[2]
        cap = jnp.full((TILE, TILE), scale, F32).astype(BF16)
        wbuf[pl.ds(LANES + 16, LANES - 16), :] = jnp.zeros((LANES - 16, own), BF16)

        load_x.wait()
        load_v.wait()
        row_idx = lax.broadcasted_iota(jnp.int32, (16, LANES), 0)
        for r in range(own // LANES):
            x_t = xbuf[0, 0, pl.ds(r * LANES, LANES), :].astype(F32).T
            norm = jnp.sum(x_t * x_t, axis=0, keepdims=True) * shrink2
            parts = [jnp.broadcast_to(p, (16, LANES)) for p in split3(norm)]
            vis = jnp.where(row_idx < 6, 1.0, 0.0)
            mine = jnp.where(row_idx < 3, -1.0, 0.0)
            for i, part in enumerate(parts):
                vis = jnp.where(row_idx == i, part, vis)
                mine = jnp.where(row_idx == i + 3, -part, mine)
            vbuf[0, 0, pl.ds(16, 16), pl.ds(r * LANES, LANES)] = vis.astype(BF16)
            wbuf[pl.ds(0, LANES), pl.ds(r * LANES, LANES)] = (x_t * (2.0 * shrink2)).astype(BF16)
            wbuf[pl.ds(LANES, 16), pl.ds(r * LANES, LANES)] = mine.astype(BF16)

        def wave_copies(wave):
            rel, src, _, _ = WAVES[wave]
            copies = []
            for d in range(4):
                q = (d + rel) % 4
                target = chip_id(*STEP[d])
                rows = pl.ds(q * quarter, quarter)
                copies.append(pltpu.make_async_remote_copy(
                    xbuf.at[0, src, rows], xbuf.at[0, wave + 1, rows], send_sem.at[wave % AHEAD, q, 0], recv_sem.at[wave, q, 0], device_id=target))
                copies.append(pltpu.make_async_remote_copy(
                    vbuf.at[0, src, :, rows], vbuf.at[0, wave + 1, :, rows], send_sem.at[wave % AHEAD, q, 1], recv_sem.at[wave, q, 1], device_id=target))
            return copies

        def piece_copies(slot):
            copies = []
            for q in range(4):
                rows = pl.ds(q * quarter, quarter)
                sem = (slot - 1) % AHEAD
                copies.append(pltpu.make_async_remote_copy(
                    xbuf.at[0, slot, rows], xbuf.at[0, slot, rows], send_sem.at[sem, q, 0], recv_sem.at[slot - 1, q, 0], device_id=sibling))
                copies.append(pltpu.make_async_remote_copy(
                    vbuf.at[0, slot, :, rows], vbuf.at[0, slot, :, rows], send_sem.at[sem, q, 1], recv_sem.at[slot - 1, q, 1], device_id=sibling))
            return copies

        def sibling_copies(slot):
            return (
                pltpu.make_async_remote_copy(xbuf.at[0, slot], xbuf.at[1, slot], sib_send.at[0], sib_recv.at[slot, 0], device_id=sibling),
                pltpu.make_async_remote_copy(vbuf.at[0, slot], vbuf.at[1, slot], sib_send.at[1], sib_recv.at[slot, 1], device_id=sibling),
            )

        def y_piece_copy(slot, q, target):
            rows = pl.ds(q * quarter, quarter)
            return pltpu.make_async_remote_copy(
                ybuf.at[0, 0, :, rows], ybuf.at[0, slot, :, rows], ysend_sem.at[slot - 1, q], yrecv_sem.at[slot - 1, q], device_id=target)

        def y_sibling_copy(slot, chain):
            return pltpu.make_async_remote_copy(ybuf.at[0, slot], ybuf.at[1, slot], ysib_send.at[chain], ysib_recv.at[slot], device_id=sibling)

        def spill(idx):
            return pltpu.make_async_copy(tbuf.at[idx % RING], store_ref.at[idx], spill_sem.at[idx % RING])

        def fetch(idx):
            return pltpu.make_async_copy(store_ref.at[idx], tbuf.at[idx % RING], fetch_sem.at[idx % RING])

        def widen(which, slot, r):
            for lane in range(r * TILE, (r + 1) * TILE, LANES):
                rows = vbuf[which, slot, pl.ds(16, 16), pl.ds(lane, LANES)].astype(F32)
                full = jnp.concatenate([rows, jnp.zeros((LANES - 16, LANES), F32)], axis=0)
                abuf[which, pl.ds(lane, LANES), :] = full.T.astype(BF16)

        def first_block(which, slot):
            idx = 2 * slot + which
            kept = idx // n_far
            place = (idx % RING) * (1 - kept) + (idx - n_far + RING) * kept

            @pl.when((idx >= RING) & (idx < n_far))
            def _():
                spill(idx - RING).wait()

            gram, part = {}, None
            widen(which, slot, 0)
            for u in range(n_u + LAG):
                if u + 1 < n_r:
                    widen(which, slot, u + 1)
                if u < n_u:
                    c, r = units[u]
                    rows = pl.ds(r * TILE, TILE)
                    lhs = jnp.concatenate([xbuf[which, slot, rows, :], abuf[which, rows, :]], axis=1)
                    gram[u] = jnp.dot(lhs, wbuf[:, pl.ds(c * TILE, TILE)], preferred_element_type=F32)
                if u >= LAG:
                    c, r = units[u - LAG]
                    tile = jnp.minimum((jnp.exp2(gram.pop(u - LAG) * coef) * scale).astype(BF16), cap)
                    tbuf[place, pl.ds(r * TILE, TILE), pl.ds(c * TILE, TILE)] = tile
                    v_rows = vbuf[which, slot, pl.ds(0, 16), pl.ds(r * TILE, TILE)]
                    kept_tile = tbuf[place, pl.ds(r * TILE, TILE), pl.ds(c * TILE, TILE)]
                    prod = jnp.dot(jnp.concatenate([v_rows] * (PAD // 16), axis=0), kept_tile, preferred_element_type=F32)
                    part = prod if r == 0 else part + prod
                    if r == n_r - 1:
                        total[:, pl.ds(c * TILE, TILE)] += part

            @pl.when(idx < n_far)
            def _():
                spill(idx).start()

        def second_block(place, which, slot):
            for c in range(n_c):
                cols = pl.ds(c * TILE, TILE)
                total[pl.ds(0, 16), cols] += jnp.dot(ybuf[which, slot], tbuf[place, :, cols], preferred_element_type=F32)

        total[...] = jnp.zeros_like(total)
        pl.semaphore_wait(barrier, n_slot)
        for copy in sibling_copies(0):
            copy.start()
        for wave in range(AHEAD):
            for copy in wave_copies(wave):
                copy.start()

        def first_step(slot, carry):
            @pl.when(slot > 0)
            def _():
                for copy in piece_copies(slot):
                    copy.wait()
                for copy in sibling_copies(slot):
                    copy.wait_send()
                    copy.start()

            for wave in range(AHEAD, n_slot - 1):
                @pl.when(slot == wave - AHEAD + 1)
                def _():
                    for copy in wave_copies(wave):
                        copy.start()

            @pl.when(slot == n_slot - KEPT_SLOTS)
            def _():
                for idx in range(RING):
                    spill(n_far - RING + idx).wait()
                for idx in range(RING):
                    fetch(idx).start()

            first_block(0, slot)
            for copy in sibling_copies(slot):
                copy.wait_recv()
            first_block(1, slot)
            return carry

        lax.fori_loop(0, n_slot, first_step, 0)
        ybuf[0, 0] = total[pl.ds(0, 16), :].astype(BF16)
        total[...] = jnp.zeros_like(total)
        for copy in sibling_copies(n_slot - 1):
            copy.wait_send()

        y_sibling_copy(0, 0).start()
        for wave, (_, _, prim, sec) in enumerate(WAVES):
            for q in range(4):
                (px, py), (sx, sy) = STEP[q], STEP[(q + 1) % 4]
                y_piece_copy(wave + 1, q, chip_id((prim * px + sec * sx) % side, (prim * py + sec * sy) % side)).start()

        n_far_slots = n_slot - KEPT_SLOTS

        def far_block(which, slot):
            idx = 2 * slot + which
            fetch(idx).wait()
            second_block(idx % RING, which, slot)

            @pl.when(idx + RING < n_far)
            def _():
                fetch(idx + RING).start()

        def pass_on(slot, chain):
            for q in range(4):
                y_piece_copy(slot, q, sibling).wait()
            y_sibling_copy(slot, chain).start()

        def second_step(slot, carry):
            @pl.when(slot > 0)
            def _():
                y_sibling_copy(slot, 0).wait_send()
                pass_on(slot, 0)

            far_block(0, slot)
            y_sibling_copy(slot, 0).wait_recv()
            far_block(1, slot)
            near = slot - (n_far_slots - 2 * KEPT_SLOTS)
            near_slot = n_far_slots + near // 2

            @pl.when((near >= 0) & (near % 2 == 0))
            def _():
                pass_on(near_slot, 1)
                second_block(RING + near, 0, near_slot)

            @pl.when((near >= 0) & (near % 2 == 1))
            def _():
                y_sibling_copy(near_slot, 1).wait_send()
                y_sibling_copy(near_slot, 1).wait_recv()
                second_block(RING + near, 1, near_slot)

            return carry

        lax.fori_loop(0, n_far_slots, second_step, 0)
        out_ref[...] = total[pl.ds(0, 16), :]
        y_sibling_copy(n_far_slots - 1, 0).wait_send()

    return kernel, n_slot


def both_passes(n_row, scal, x_loc, vt_loc):
    own, feat = x_loc.shape
    n_col = vt_loc.shape[0]
    kernel, n_slot = make_kernel(n_row, own)
    dma = pltpu.SemaphoreType.DMA
    return pl.pallas_call(
        kernel,
        in_specs=[pl.BlockSpec(memory_space=pltpu.SMEM), pl.BlockSpec(memory_space=pl.ANY), pl.BlockSpec(memory_space=pl.ANY)],
        out_specs=[pl.BlockSpec(memory_space=pltpu.VMEM), pl.BlockSpec(memory_space=pl.ANY)],
        out_shape=[jax.ShapeDtypeStruct((n_col, own), F32), jax.ShapeDtypeStruct((2 * (n_slot - KEPT_SLOTS), own, own), BF16)],
        scratch_shapes=[
            pltpu.VMEM((2, n_slot, own, feat), BF16),
            pltpu.VMEM((2, own, feat), BF16),
            pltpu.VMEM((2, n_slot, 32, own), BF16),
            pltpu.VMEM((2, n_slot, n_col, own), BF16),
            pltpu.VMEM((2 * feat, own), BF16),
            pltpu.VMEM((PAD, own), F32),
            pltpu.VMEM((RING + 2 * KEPT_SLOTS, own, own), BF16),
            dma((2,)),
            dma((AHEAD, 4, 2)),
            dma((n_slot - 1, 4, 2)),
            dma((2,)),
            dma((n_slot, 2)),
            dma((n_slot - 1, 4)),
            dma((n_slot - 1, 4)),
            dma((2,)),
            dma((n_slot,)),
            dma((RING,)),
            dma((RING,)),
        ],
        compiler_params=pltpu.CompilerParams(collective_id=0, has_side_effects=True, vmem_limit_bytes=67000000),
        name="both_passes",
    )(scal, x_loc, vt_loc)[0]


def solution(mesh):
    def local_program(x_loc, v_loc, length_scale, out_scale):
        ell, scale = length_scale[0], out_scale[0]
        shrink = jnp.where(ell > 2.0**64, 2.0**-70, jnp.where(ell > 2.0**32, 2.0**-32, 1.0)).astype(F32)
        ell = ell * shrink
        scal = jnp.stack([LOG2E / (2.0 * ell * ell), scale, shrink * shrink])
        return both_passes(mesh.shape["row"], scal, x_loc, v_loc.T).T

    row_spec = P(("task", "row"), None)
    return jax.shard_map(local_program, mesh=mesh, in_specs=(row_spec, row_spec, P("task"), P("task")), out_specs=row_spec, check_vma=False)
```

```python
import math

import jax
import jax.numpy as jnp
from jax import lax
from jax.experimental import pallas as pl
from jax.experimental.pallas import tpu as pltpu
from jax.sharding import PartitionSpec as P

BF16 = jnp.bfloat16
F32 = jnp.float32
LOG2E = 1.4426950408889634
TILE = 512
LANES = 128
LAG = 1
PAD = 96
STEP = ((1, 0), (0, 1), (-1, 0), (0, -1))
WAVES = (
    (0, 0, 1, 0),
    (2, 0, -1, 0),
    (3, 0, 0, 1),
    (1, 0, 0, -1),
    (0, 1, 2, 0),
    (3, 1, 1, 1),
    (1, 1, 1, -1),
    (3, 2, -1, 1),
    (1, 2, -1, -1),
    (3, 3, 0, 2),
    (3, 5, 2, 1),
    (1, 5, 2, -1),
    (3, 6, 1, 2),
    (3, 8, -1, 2),
    (3, 11, 2, 2),
)
AHEAD = 4
RING = 3
KEPT_SLOTS = 3
REDO_SLOTS = 1


def split3(val):
    high = val.astype(BF16).astype(F32)
    mid = (val - high).astype(BF16).astype(F32)
    low = (val - high) - mid
    return high, mid, low


def make_kernel(n_row, own):
    side = math.isqrt(n_row // 2)
    n_slot = side * side
    quarter = own // 4
    n_c, n_r = own // TILE, own // TILE
    n_far_slots = n_slot - KEPT_SLOTS - REDO_SLOTS
    n_far, n_ring = 2 * n_far_slots, 2 * (n_slot - KEPT_SLOTS)
    units = [(c, r) for c in range(n_c) for r in range(n_r)]
    n_u = len(units)

    def kernel(
        scal_ref, x_ref, vt_ref, out_ref, store_ref, xbuf, abuf, vbuf, ybuf, wbuf, total, tbuf,
        load_sem, send_sem, recv_sem, sib_send, sib_recv, ysend_sem, yrecv_sem, ysib_send, ysib_recv, spill_sem, fetch_sem,
    ):
        me = lax.axis_index("row")
        core, chip = me % 2, me // 2
        cx, cy = chip % side, chip // side

        def chip_id(dx, dy):
            return {"row": (((cy + dy + side) % side) * side + (cx + dx + side) % side) * 2 + core}

        sibling = {"row": chip * 2 + 1 - core}

        load_x = pltpu.make_async_copy(x_ref, xbuf.at[0, 0], load_sem.at[0])
        load_v = pltpu.make_async_copy(vt_ref, vbuf.at[0, 0, pl.ds(0, 16)], load_sem.at[1])
        load_x.start()
        load_v.start()

        barrier = pltpu.get_barrier_semaphore()
        for k in range(1, n_slot):
            pl.semaphore_signal(barrier, inc=1, device_id=chip_id(k % side, k // side))
        pl.semaphore_signal(barrier, inc=1, device_id=sibling)

        coef, scale, shrink2 = scal_ref[0], scal_ref[1], scal_ref[2]
        cap = jnp.full((TILE, TILE), scale, F32).astype(BF16)
        wbuf[pl.ds(LANES + 16, LANES - 16), :] = jnp.zeros((LANES - 16, own), BF16)

        def wave_copies(wave):
            rel, src, _, _ = WAVES[wave]
            copies = []
            for d in range(4):
                q = (d + rel) % 4
                target = chip_id(*STEP[d])
                rows = pl.ds(q * quarter, quarter)
                copies.append(pltpu.make_async_remote_copy(
                    xbuf.at[0, src, rows], xbuf.at[0, wave + 1, rows], send_sem.at[wave % AHEAD, q, 0], recv_sem.at[wave, q, 0], device_id=target))
                copies.append(pltpu.make_async_remote_copy(
                    vbuf.at[0, src, :, rows], vbuf.at[0, wave + 1, :, rows], send_sem.at[wave % AHEAD, q, 1], recv_sem.at[wave, q, 1], device_id=target))
            return copies

        def piece_copies(slot):
            copies = []
            for q in range(4):
                rows = pl.ds(q * quarter, quarter)
                sem = (slot - 1) % AHEAD
                copies.append(pltpu.make_async_remote_copy(
                    xbuf.at[0, slot, rows], xbuf.at[0, slot, rows], send_sem.at[sem, q, 0], recv_sem.at[slot - 1, q, 0], device_id=sibling))
                copies.append(pltpu.make_async_remote_copy(
                    vbuf.at[0, slot, :, rows], vbuf.at[0, slot, :, rows], send_sem.at[sem, q, 1], recv_sem.at[slot - 1, q, 1], device_id=sibling))
            return copies

        def sibling_copies(slot):
            return (
                pltpu.make_async_remote_copy(xbuf.at[0, slot], xbuf.at[1, slot], sib_send.at[0], sib_recv.at[slot, 0], device_id=sibling),
                pltpu.make_async_remote_copy(vbuf.at[0, slot], vbuf.at[1, slot], sib_send.at[1], sib_recv.at[slot, 1], device_id=sibling),
            )

        def y_piece_copy(slot, q, target):
            rows = pl.ds(q * quarter, quarter)
            return pltpu.make_async_remote_copy(
                ybuf.at[0, 0, :, rows], ybuf.at[0, slot, :, rows], ysend_sem.at[slot - 1, q], yrecv_sem.at[slot - 1, q], device_id=target)

        def y_sibling_copy(slot, chain):
            return pltpu.make_async_remote_copy(ybuf.at[0, slot], ybuf.at[1, slot], ysib_send.at[chain], ysib_recv.at[slot], device_id=sibling)

        def spill(idx):
            return pltpu.make_async_copy(tbuf.at[idx % RING], store_ref.at[idx], spill_sem.at[idx % RING])

        def fetch(idx):
            return pltpu.make_async_copy(store_ref.at[idx], tbuf.at[idx % RING], fetch_sem.at[idx % RING])

        def widen(which, slot, r):
            for lane in range(r * TILE, (r + 1) * TILE, LANES):
                rows = vbuf[which, slot, pl.ds(16, 16), pl.ds(lane, LANES)].astype(F32)
                full = jnp.concatenate([rows, jnp.zeros((LANES - 16, LANES), F32)], axis=0)
                abuf[which, pl.ds(lane, LANES), :] = full.T.astype(BF16)

        def tiles(buf, which, slot, place):
            gram, part = {}, None
            widen(which, slot, 0)
            for u in range(n_u + LAG):
                if u + 1 < n_r:
                    widen(which, slot, u + 1)
                if u < n_u:
                    c, r = units[u]
                    rows = pl.ds(r * TILE, TILE)
                    lhs = jnp.concatenate([xbuf[which, slot, rows, :], abuf[which, rows, :]], axis=1)
                    gram[u] = jnp.dot(lhs, wbuf[:, pl.ds(c * TILE, TILE)], preferred_element_type=F32)
                if u >= LAG:
                    c, r = units[u - LAG]
                    tile = jnp.minimum((jnp.exp2(gram.pop(u - LAG) * coef) * scale).astype(BF16), cap)
                    if place is not None:
                        tbuf[place, pl.ds(r * TILE, TILE), pl.ds(c * TILE, TILE)] = tile
                        tile = tbuf[place, pl.ds(r * TILE, TILE), pl.ds(c * TILE, TILE)]
                    v_rows = buf[which, slot, pl.ds(0, 16), pl.ds(r * TILE, TILE)]
                    prod = jnp.dot(jnp.concatenate([v_rows] * (PAD // 16), axis=0), tile, preferred_element_type=F32)
                    part = prod if r == 0 else part + prod
                    if r == n_r - 1:
                        total[:, pl.ds(c * TILE, TILE)] += part

        def first_block(which, slot):
            idx = 2 * slot + which
            kept = idx // n_ring
            place = (idx % RING) * (1 - kept) + (idx - n_ring + RING) * kept

            @pl.when((idx >= RING) & (idx < min(n_far + RING, n_ring)))
            def _():
                spill(idx - RING).wait()

            tiles(vbuf, which, slot, place)

            @pl.when(idx < n_far)
            def _():
                spill(idx).start()

        def second_block(place, which, slot):
            for c in range(n_c):
                cols = pl.ds(c * TILE, TILE)
                total[pl.ds(0, 16), cols] += jnp.dot(ybuf[which, slot], tbuf[place, :, cols], preferred_element_type=F32)

        load_x.wait()
        pl.semaphore_wait(barrier, n_slot)
        outgoing = [sibling_copies(0)] + [wave_copies(wave) for wave in range(AHEAD)]
        for copies in outgoing[:2]:
            for copy in copies[0::2]:
                copy.start()
        load_v.wait()
        row_idx = lax.broadcasted_iota(jnp.int32, (16, LANES), 0)
        for r in range(own // LANES):
            x_t = xbuf[0, 0, pl.ds(r * LANES, LANES), :].astype(F32).T
            norm = jnp.sum(x_t * x_t, axis=0, keepdims=True) * shrink2
            parts = [jnp.broadcast_to(p, (16, LANES)) for p in split3(norm)]
            vis = jnp.where(row_idx < 6, 1.0, 0.0)
            mine = jnp.where(row_idx < 3, -1.0, 0.0)
            for i, part in enumerate(parts):
                vis = jnp.where(row_idx == i, part, vis)
                mine = jnp.where(row_idx == i + 3, -part, mine)
            vbuf[0, 0, pl.ds(16, 16), pl.ds(r * LANES, LANES)] = vis.astype(BF16)
            wbuf[pl.ds(0, LANES), pl.ds(r * LANES, LANES)] = (x_t * (2.0 * shrink2)).astype(BF16)
            wbuf[pl.ds(LANES, 16), pl.ds(r * LANES, LANES)] = mine.astype(BF16)

        for i, copies in enumerate(outgoing):
            for copy in copies[1::2] if i < 2 else copies:
                copy.start()
        total[...] = jnp.zeros_like(total)

        def first_step(slot, carry):
            @pl.when(slot > 0)
            def _():
                for copy in piece_copies(slot):
                    copy.wait()
                for copy in sibling_copies(slot):
                    copy.wait_send()
                    copy.start()

            for wave in range(AHEAD, n_slot - 1):
                @pl.when(slot == wave - AHEAD + 1)
                def _():
                    for copy in wave_copies(wave):
                        copy.start()

            @pl.when(slot == n_slot - KEPT_SLOTS)
            def _():
                for idx in range(n_ring, n_far + RING):
                    spill(idx - RING).wait()
                for idx in range(RING):
                    fetch(idx).start()

            first_block(0, slot)
            for copy in sibling_copies(slot):
                copy.wait_recv()
            first_block(1, slot)
            return carry

        lax.fori_loop(0, n_slot, first_step, 0)
        ybuf[0, 0] = total[pl.ds(0, 16), :].astype(BF16)
        total[...] = jnp.zeros_like(total)
        for copy in sibling_copies(n_slot - 1):
            copy.wait_send()

        y_sibling_copy(0, 0).start()
        for wave, (_, _, prim, sec) in enumerate(WAVES):
            for q in range(4):
                (px, py), (sx, sy) = STEP[q], STEP[(q + 1) % 4]
                y_piece_copy(wave + 1, q, chip_id((prim * px + sec * sx) % side, (prim * py + sec * sy) % side)).start()


        def far_block(which, slot):
            idx = 2 * slot + which
            fetch(idx).wait()
            second_block(idx % RING, which, slot)

            @pl.when(idx + RING < n_far)
            def _():
                fetch(idx + RING).start()

        def pass_on(slot, chain):
            for q in range(4):
                y_piece_copy(slot, q, sibling).wait()
            y_sibling_copy(slot, chain).start()

        def second_step(slot, carry):
            @pl.when(slot > 0)
            def _():
                y_sibling_copy(slot, 0).wait_send()
                pass_on(slot, 0)

            far_block(0, slot)
            y_sibling_copy(slot, 0).wait_recv()
            far_block(1, slot)
            redo = (slot - 3) // 2
            redo_slot = n_far_slots + redo // 2

            for half in (0, 1):
                @pl.when((slot >= 3) & (slot % 2 == 1) & (redo < 2 * REDO_SLOTS) & (redo % 2 == half))
                def _():
                    if half == 0:
                        @pl.when(redo > 0)
                        def _():
                            y_sibling_copy(redo_slot, 2).wait_send()
                        pass_on(redo_slot, 2)
                    else:
                        y_sibling_copy(redo_slot, 2).wait_recv()
                    tiles(ybuf, half, redo_slot, None)

            near = slot - (n_far_slots - 2 * KEPT_SLOTS)
            near_slot = n_far_slots + REDO_SLOTS + near // 2

            @pl.when((near >= 0) & (near % 2 == 0))
            def _():
                pass_on(near_slot, 1)
                second_block(RING + near, 0, near_slot)

            @pl.when((near >= 0) & (near % 2 == 1))
            def _():
                y_sibling_copy(near_slot, 1).wait_send()
                y_sibling_copy(near_slot, 1).wait_recv()
                second_block(RING + near, 1, near_slot)

            return carry

        lax.fori_loop(0, n_far_slots, second_step, 0)
        out_ref[...] = total[pl.ds(0, 16), :]
        y_sibling_copy(n_far_slots - 1, 0).wait_send()
        y_sibling_copy(n_far_slots + REDO_SLOTS - 1, 2).wait_send()

    return kernel, n_slot


def both_passes(n_row, scal, x_loc, vt_loc):
    own, feat = x_loc.shape
    n_col = vt_loc.shape[0]
    kernel, n_slot = make_kernel(n_row, own)
    dma = pltpu.SemaphoreType.DMA
    return pl.pallas_call(
        kernel,
        in_specs=[pl.BlockSpec(memory_space=pltpu.SMEM), pl.BlockSpec(memory_space=pl.ANY), pl.BlockSpec(memory_space=pl.ANY)],
        out_specs=[pl.BlockSpec(memory_space=pltpu.VMEM), pl.BlockSpec(memory_space=pl.ANY)],
        out_shape=[jax.ShapeDtypeStruct((n_col, own), F32), jax.ShapeDtypeStruct((2 * (n_slot - KEPT_SLOTS - REDO_SLOTS), own, own), BF16)],
        scratch_shapes=[
            pltpu.VMEM((2, n_slot, own, feat), BF16),
            pltpu.VMEM((2, own, feat), BF16),
            pltpu.VMEM((2, n_slot, 32, own), BF16),
            pltpu.VMEM((2, n_slot, n_col, own), BF16),
            pltpu.VMEM((2 * feat, own), BF16),
            pltpu.VMEM((PAD, own), F32),
            pltpu.VMEM((RING + 2 * KEPT_SLOTS, own, own), BF16),
            dma((2,)),
            dma((AHEAD, 4, 2)),
            dma((n_slot - 1, 4, 2)),
            dma((2,)),
            dma((n_slot, 2)),
            dma((n_slot - 1, 4)),
            dma((n_slot - 1, 4)),
            dma((3,)),
            dma((n_slot,)),
            dma((RING,)),
            dma((RING,)),
        ],
        compiler_params=pltpu.CompilerParams(collective_id=0, has_side_effects=True, vmem_limit_bytes=67000000),
        name="both_passes",
    )(scal, x_loc, vt_loc)[0]


def solution(mesh):
    def local_program(x_loc, v_loc, length_scale, out_scale):
        ell, scale = length_scale[0], out_scale[0]
        shrink = jnp.where(ell > 2.0**64, 2.0**-70, jnp.where(ell > 2.0**32, 2.0**-32, 1.0)).astype(F32)
        ell = ell * shrink
        scal = jnp.stack([LOG2E / (2.0 * ell * ell), scale, shrink * shrink])
        return both_passes(mesh.shape["row"], scal, x_loc, v_loc.T).T

    row_spec = P(("task", "row"), None)
    return jax.shard_map(local_program, mesh=mesh, in_specs=(row_spec, row_spec, P("task"), P("task")), out_specs=row_spec, check_vma=False)
```
